8 devices in a mesh: data: 1 (over z), pp: 2 (over y), ep: 4 (over x, core).
Axes of the slice: x: 2, y: 2, z: 1, core: 2. Of those that a mesh axis runs over, the one named last changes fastest.
Arguments:
- expert_out: bfloat16 [2, 1, 384, 32, 7168], P(('data', 'pp'), None, 'ep')
- expert_id: int32 [2, 1, 1024, 8], P(('data', 'pp'), None, 'ep')
- slot_id: int32 [2, 1, 1024, 8], P(('data', 'pp'), None, 'ep')
- gate: float32 [2, 1, 1024, 8], P(('data', 'pp'), None, 'ep')
- resid: bfloat16 [2, 1, 1024, 7168], P(('data', 'pp'), None, 'ep')
- owner: int32 [2, 32], P(('data', 'pp'))
- norm_w: float32 [2, 7168], P('pp')
- w_q: bfloat16 [2, 7168, 8192], P('pp')
- w_k: bfloat16 [2, 7168, 8192], P('pp')
- w_v: bfloat16 [2, 7168, 8192], P('pp')
- w_o: bfloat16 [2, 8192, 7168], P('pp')
Outputs:
- output: bfloat16 [2, 1, 1024, 7168], P(('data', 'pp'), None, 'ep')
All inputs are finite; a program needn't handle non-finite values.
Results may differ from the reference program's by a relative error of at most 0.013573.
Values are sent between devices in bfloat16 or wider.
A program may use at most 2 GiB of HBM per device.

```python
import jax
import jax.numpy as jnp
from jax import lax

STAGES = 2
EP_DEVICES = 4
MICRO = 1
SEQ_DEV = 8
SEQ_LEN = 32
MODEL_DIM = 7168
EXPERTS = 384
TOP_K = 8
HEADS = 64
HEAD_DIM = 128
CAP_DEV = 8

SEQS = EP_DEVICES * SEQ_DEV
TOKENS = SEQS * SEQ_LEN
TOK_DEV = SEQ_DEV * SEQ_LEN
CAPACITY = EP_DEVICES * CAP_DEV
QKV_WIDTH = HEADS * HEAD_DIM
HOT_COUNT = max(1, EXPERTS // 32)
HOT_BIAS = (2000 * TOP_K) // EXPERTS
NORM_EPS = 1e-6


def draw_routing(rng_key):
    key_hot, key_score = jax.random.split(rng_key)
    hot_rank = jax.random.permutation(key_hot, EXPERTS)
    hot_bias = jnp.where(hot_rank < HOT_COUNT, HOT_BIAS, 0)
    rand_score = jax.random.randint(key_score, (STAGES, MICRO, EP_DEVICES, TOK_DEV, EXPERTS), 0, 1000)
    tok_local = jnp.arange(TOK_DEV)[:, None]
    forced = jnp.where((tok_local < CAP_DEV) & (hot_rank[None, :] == 0), 4000, 0)
    full_score = (rand_score + hot_bias + forced) * EXPERTS + jnp.arange(EXPERTS)
    chosen = lax.top_k(full_score, TOP_K)[1].astype(jnp.int32)
    n_flat = TOK_DEV * TOP_K
    flat_ids = chosen.reshape(STAGES, MICRO, EP_DEVICES, n_flat)
    flat_pos = jnp.arange(n_flat)
    sort_order = jnp.argsort(flat_ids * n_flat + flat_pos, axis=-1)
    sorted_ids = jnp.take_along_axis(flat_ids, sort_order, axis=-1)
    prev_ids = jnp.concatenate([jnp.full_like(sorted_ids[..., :1], -1), sorted_ids[..., :-1]], axis=-1)
    group_start = lax.cummax(jnp.where(sorted_ids != prev_ids, flat_pos, 0), axis=3)
    rank_sorted = flat_pos - group_start
    slot_pos = jnp.take_along_axis(rank_sorted, jnp.argsort(sort_order, axis=-1), axis=-1)
    dev_base = (jnp.arange(EP_DEVICES) * CAP_DEV)[:, None]
    slot_all = jnp.where(slot_pos < CAP_DEV, dev_base + slot_pos, -1).astype(jnp.int32)
    return chosen.reshape(STAGES, MICRO, TOKENS, TOP_K), slot_all.reshape(STAGES, MICRO, TOKENS, TOP_K)


def draw_owner(rng_key):
    key_src, key_dst = jax.random.split(rng_key)
    seq_rows = jnp.broadcast_to(jnp.arange(SEQ_DEV), (STAGES, EP_DEVICES, SEQ_DEV))
    local_perm = jax.random.permutation(key_src, seq_rows, axis=2, independent=True)
    global_ids = local_perm + (jnp.arange(EP_DEVICES) * SEQ_DEV)[:, None]
    per_pair = SEQ_DEV // EP_DEVICES
    global_ids = global_ids.reshape(STAGES, EP_DEVICES, EP_DEVICES, per_pair).transpose(0, 2, 1, 3).reshape(STAGES, EP_DEVICES, SEQ_DEV)
    shuffle = jax.random.permutation(key_dst, seq_rows, axis=2, independent=True)
    owned = jnp.take_along_axis(global_ids, shuffle, axis=2)
    return owned.reshape(STAGES, SEQS).astype(jnp.int32)


def setup_inputs(seed: int = 0, part: int = 0) -> dict:
    part_key = jax.random.fold_in(jax.random.key(seed), part)
    keys_data = jax.random.split(part_key, 8)
    keys_weight = jax.random.split(jax.random.key(seed + 1), 6)
    expert_id, slot_id = draw_routing(keys_data[0])
    owner = draw_owner(keys_data[1])
    expert_scale = jnp.exp(0.7 * jax.random.normal(keys_data[2], (STAGES, MICRO, EXPERTS, 1, 1), jnp.float32))
    expert_out = (jax.random.normal(keys_data[3], (STAGES, MICRO, EXPERTS, CAPACITY, MODEL_DIM), jnp.float32) * expert_scale).astype(jnp.bfloat16)
    gate_raw = jnp.exp(1.2 * jax.random.normal(keys_data[4], (STAGES, MICRO, TOKENS, TOP_K), jnp.float32))
    gate_level = 0.5 + jax.random.uniform(keys_data[5], (STAGES, MICRO, TOKENS, 1), jnp.float32)
    gate = gate_raw / jnp.sum(gate_raw, axis=-1, keepdims=True) * gate_level
    resid = jax.random.normal(keys_data[6], (STAGES, MICRO, TOKENS, MODEL_DIM), jnp.float32).astype(jnp.bfloat16)
    norm_w = jax.random.uniform(keys_weight[0], (STAGES, MODEL_DIM), jnp.float32, 0.5, 1.5)
    qk_scale = 1.5 * MODEL_DIM ** -0.5
    w_q = (jax.random.normal(keys_weight[1], (STAGES, MODEL_DIM, QKV_WIDTH), jnp.float32) * qk_scale).astype(jnp.bfloat16)
    w_k = (jax.random.normal(keys_weight[2], (STAGES, MODEL_DIM, QKV_WIDTH), jnp.float32) * qk_scale).astype(jnp.bfloat16)
    w_v = (jax.random.normal(keys_weight[3], (STAGES, MODEL_DIM, QKV_WIDTH), jnp.float32) * MODEL_DIM ** -0.5).astype(jnp.bfloat16)
    w_o = (jax.random.normal(keys_weight[4], (STAGES, QKV_WIDTH, MODEL_DIM), jnp.float32) * QKV_WIDTH ** -0.5).astype(jnp.bfloat16)
    return dict(expert_out=expert_out, expert_id=expert_id, slot_id=slot_id, gate=gate, resid=resid, owner=owner, norm_w=norm_w, w_q=w_q, w_k=w_k, w_v=w_v, w_o=w_o)


def attend_block(y_seq, norm_scale, w_q_stage, w_k_stage, w_v_stage, w_o_stage):
    y_f32 = y_seq.astype(jnp.float32)
    inv_rms = lax.rsqrt(jnp.mean(y_f32 * y_f32, axis=-1, keepdims=True) + NORM_EPS)
    normed = (y_f32 * inv_rms * norm_scale).astype(jnp.bfloat16)
    queries = jnp.dot(normed, w_q_stage, preferred_element_type=jnp.float32).astype(jnp.bfloat16).reshape(SEQ_LEN, HEADS, HEAD_DIM)
    key_vecs = jnp.dot(normed, w_k_stage, preferred_element_type=jnp.float32).astype(jnp.bfloat16).reshape(SEQ_LEN, HEADS, HEAD_DIM)
    values = jnp.dot(normed, w_v_stage, preferred_element_type=jnp.float32).astype(jnp.bfloat16).reshape(SEQ_LEN, HEADS, HEAD_DIM)
    scores = jnp.einsum('qhe,khe->hqk', queries.astype(jnp.float32), key_vecs.astype(jnp.float32)) * HEAD_DIM ** -0.5
    causal = jnp.arange(SEQ_LEN)[:, None] >= jnp.arange(SEQ_LEN)[None, :]
    attn_probs = jax.nn.softmax(jnp.where(causal, scores, -1e30), axis=-1).astype(jnp.bfloat16)
    head_mix = jnp.einsum('hqk,khe->qhe', attn_probs.astype(jnp.float32), values.astype(jnp.float32)).astype(jnp.bfloat16).reshape(SEQ_LEN, QKV_WIDTH)
    out_proj = jnp.dot(head_mix, w_o_stage, preferred_element_type=jnp.float32).astype(jnp.bfloat16)
    return (y_f32 + out_proj.astype(jnp.float32)).astype(jnp.bfloat16)


def reference(expert_out, expert_id, slot_id, gate, resid, owner, norm_w, w_q, w_k, w_v, w_o):
    from_prev = tuple(jnp.roll(arr_in, 1, axis=0) for arr_in in (expert_out, expert_id, slot_id, gate, resid))

    def per_stage(stage_args):
        out_s, ids_s, slots_s, gate_s, resid_s, owner_s, norm_s, w_q_s, w_k_s, w_v_s, w_o_s = stage_args

        def per_micro(micro_args):
            out_m, ids_m, slots_m, gate_m, resid_m = micro_args
            flat_out = out_m.reshape(EXPERTS * CAPACITY, MODEL_DIM)

            def per_seq(seq_index):
                seq_start = seq_index * SEQ_LEN
                ids_q = lax.dynamic_slice_in_dim(ids_m, seq_start, SEQ_LEN, 0)
                slots_q = lax.dynamic_slice_in_dim(slots_m, seq_start, SEQ_LEN, 0)
                gate_q = lax.dynamic_slice_in_dim(gate_m, seq_start, SEQ_LEN, 0)
                resid_q = lax.dynamic_slice_in_dim(resid_m, seq_start, SEQ_LEN, 0)
                kept_mask = slots_q >= 0
                row_index = ids_q * CAPACITY + jnp.where(kept_mask, slots_q, 0)
                picked = flat_out[row_index].astype(jnp.float32)
                weights = jnp.where(kept_mask, gate_q, 0.0)
                combined = jnp.einsum('lk,lkd->ld', weights, picked)
                y_seq = (resid_q.astype(jnp.float32) + combined).astype(jnp.bfloat16)
                return attend_block(y_seq, norm_s, w_q_s, w_k_s, w_v_s, w_o_s)

            return lax.map(per_seq, owner_s)

        return lax.map(per_micro, (out_s, ids_s, slots_s, gate_s, resid_s))

    result = lax.map(per_stage, from_prev + (owner, norm_w, w_q, w_k, w_v, w_o))
    return result.reshape(STAGES, MICRO, TOKENS, MODEL_DIM)
```

```python
import functools

import jax
import jax.numpy as jnp
from jax import lax
from jax.experimental import pallas as pl
from jax.experimental.pallas import tpu as pltpu
from jax.sharding import PartitionSpec as P

HEAD_DIM = 128
NORM_EPS = 1e-6
F32, BF16 = jnp.float32, jnp.bfloat16
MESH = pl.DeviceIdType.MESH
VMEM_LIMIT = 66_000_000


def combine_kernel(n_ep, n_stages, dk, nk, o_hbm, info_ref, h_hbm, y_hbm, obuf, hbuf, w3, perm, send_a, recv_a, keep, send_b, recv_b,
                   send_c, o_sem, h_sem, sa_sem, ra_sem, sb_sem, rb_sem, sc_sem, rc_sem):
    me = lax.axis_index('ep')
    rank = lax.axis_index('pp')
    core_peer = me + 1 - 2 * lax.rem(me, 2)
    x_peer = lax.rem(me + 2, n_ep)
    next_rank = lax.rem(rank + 1, n_stages)
    prev_rank = lax.rem(rank + n_stages - 1, n_stages)
    n_exp, cap_dev, n_slot = obuf.shape[1], obuf.shape[2], w3.shape[-1]
    n_tok = h_hbm.shape[0]
    n_dest = n_tok // n_ep

    def o_copy(k, o):
        j = lax.rem(me + o, n_ep)
        return pltpu.make_async_copy(o_hbm.at[:, pl.ds(pl.multiple_of(j * cap_dev, cap_dev), cap_dev), pl.ds(pl.multiple_of(k * dk, dk), dk)],
                                     obuf.at[o], o_sem.at[o])

    def h_copy(k):
        return pltpu.make_async_copy(h_hbm.at[:, pl.ds(pl.multiple_of(k * dk, dk), dk)], hbuf, h_sem.at[0])

    def a_copy(k):
        return pltpu.make_async_remote_copy(send_a.at[lax.rem(k, 2)], recv_a.at[k], sa_sem.at[lax.rem(k, 2)], ra_sem.at[k],
                                            device_id={'ep': core_peer}, device_id_type=MESH)

    def b_copy(k):
        return pltpu.make_async_remote_copy(send_b.at[lax.rem(k, 4)], recv_b.at[k], sb_sem.at[lax.rem(k, 4)], rb_sem.at[k],
                                            device_id={'ep': x_peer}, device_id_type=MESH)

    def c_copy(k):
        return pltpu.make_async_remote_copy(send_c.at[lax.rem(k, 2)], y_hbm.at[:, pl.ds(pl.multiple_of(k * dk, dk), dk)], sc_sem.at[lax.rem(k, 2)],
                                            rc_sem.at[k], device_id={'pp': next_rank}, device_id_type=MESH)

    for o in range(n_ep):
        o_copy(0, o).start()
    h_copy(0).start()

    barrier = pltpu.get_barrier_semaphore()
    pl.semaphore_signal(barrier, inc=1, device_id={'ep': core_peer}, device_id_type=MESH)
    pl.semaphore_signal(barrier, inc=1, device_id={'ep': x_peer}, device_id_type=MESH)
    pl.semaphore_signal(barrier, inc=1, device_id={'pp': prev_rank}, device_id_type=MESH)

    rb = 32

    def build(step, _):
        o = step // (n_tok // rb)
        row = pl.multiple_of(lax.rem(step, n_tok // rb) * rb, rb)
        rows = info_ref[lax.rem(me + o, n_ep), pl.ds(row, rb), :]
        slot = lax.broadcasted_iota(jnp.int32, (rb, n_slot), 1).astype(F32)
        w = jnp.zeros((rb, n_slot), F32)
        for c in range(8):
            w = jnp.where(rows[:, c:c + 1] == slot, rows[:, 8 + c:9 + c], w)
        high = w.astype(BF16)
        rest = w - high.astype(F32)
        mid = rest.astype(BF16)
        w3[o, 0, pl.ds(row, rb), :] = high
        w3[o, 1, pl.ds(row, rb), :] = mid
        w3[o, 2, pl.ds(row, rb), :] = (rest - mid.astype(F32)).astype(BF16)
        return 0

    lax.fori_loop(0, n_ep * (n_tok // rb), build, 0)
    home = info_ref[me, :, 16:17]
    perm[...] = (home == lax.broadcasted_iota(jnp.int32, (n_tok, n_tok), 1).astype(F32)).astype(F32).astype(BF16)
    pl.semaphore_wait(barrier, 3)

    def partial_sums(k):
        @pl.when(k >= 2)
        def _():
            a_copy(k - 2).wait_send()

        @pl.when(k >= 4)
        def _():
            b_copy(k - 4).wait_send()

        for o in range(n_ep):
            o_copy(k, o).wait()
            rows = obuf[o].reshape(n_exp * cap_dev, dk)
            part = jnp.dot(w3[o, 0], rows, preferred_element_type=F32)
            part += jnp.dot(w3[o, 1], rows, preferred_element_type=F32)
            part += jnp.dot(w3[o, 2], rows, preferred_element_type=F32)
            if o == 0:
                h_copy(k).wait()
                part += jnp.dot(perm[...], hbuf[...], preferred_element_type=F32)
            place = pl.ds(pl.multiple_of(lax.rem(me + o, n_ep) * n_dest, n_dest), n_dest)
            keep[lax.rem(k, 4), place, :] = part[0:n_dest]
            send_b[lax.rem(k, 4), place, :] = part[n_dest:2 * n_dest]
            send_a[lax.rem(k, 2), 0, place, :] = part[2 * n_dest:3 * n_dest]
            send_a[lax.rem(k, 2), 1, place, :] = part[3 * n_dest:4 * n_dest]

            @pl.when(k + 1 < nk)
            def _():
                o_copy(k + 1, o).start()
                if o == 0:
                    h_copy(k + 1).start()

        a_copy(k).start()

    def across_x(k):
        a_copy(k).wait_recv()
        keep[lax.rem(k, 4)] = keep[lax.rem(k, 4)] + recv_a[k, 0]
        send_b[lax.rem(k, 4)] = send_b[lax.rem(k, 4)] + recv_a[k, 1]
        b_copy(k).start()

    def across_y(k):
        b_copy(k).wait_recv()

        @pl.when(k >= 2)
        def _():
            c_copy(k - 2).wait_send()

        send_c[lax.rem(k, 2)] = (keep[lax.rem(k, 4)] + recv_b[k]).astype(BF16)
        c_copy(k).start()

    def step(k, _):
        @pl.when(k < nk)
        def _():
            partial_sums(k)

        @pl.when((k >= 1) & (k < nk + 1))
        def _():
            across_x(k - 1)

        @pl.when(k >= 3)
        def _():
            across_y(k - 3)

        return 0

    lax.fori_loop(0, nk + 3, step, 0)

    for k in range(nk - 2, nk):
        a_copy(k).wait_send()
        c_copy(k).wait_send()
    for k in range(nk - 4, nk):
        b_copy(k).wait_send()

    def arrive(k, _):
        c_copy(k).wait_recv()
        return 0

    lax.fori_loop(0, nk, arrive, 0)


def combine_and_send(out_local, info, resid, n_ep, n_stages, dk=512):
    n_exp, capacity, dim = out_local.shape
    n_tok = resid.shape[0]
    cap_dev = capacity // n_ep
    n_slot = n_exp * cap_dev
    nk = dim // dk
    any_spec = pl.BlockSpec(memory_space=pl.ANY)
    dma = pltpu.SemaphoreType.DMA
    return pl.pallas_call(
        functools.partial(combine_kernel, n_ep, n_stages, dk, nk),
        out_shape=jax.ShapeDtypeStruct((n_tok, dim), BF16),
        in_specs=[any_spec, pl.BlockSpec(memory_space=pltpu.VMEM), any_spec],
        out_specs=any_spec,
        scratch_shapes=[
            pltpu.VMEM((n_ep, n_exp, cap_dev, dk), BF16),
            pltpu.VMEM((n_tok, dk), BF16),
            pltpu.VMEM((n_ep, 3, n_tok, n_slot), BF16),
            pltpu.VMEM((n_tok, n_tok), BF16),
            pltpu.VMEM((2, 2, n_tok, dk), F32),
            pltpu.VMEM((nk, 2, n_tok, dk), F32),
            pltpu.VMEM((4, n_tok, dk), F32),
            pltpu.VMEM((4, n_tok, dk), F32),
            pltpu.VMEM((nk, n_tok, dk), F32),
            pltpu.VMEM((2, n_tok, dk), BF16),
            dma((n_ep,)), dma((1,)), dma((2,)), dma((nk,)), dma((4,)), dma((nk,)), dma((2,)), dma((nk,)),
        ],
        compiler_params=pltpu.CompilerParams(collective_id=0, has_side_effects=True, vmem_limit_bytes=VMEM_LIMIT),
        name='combine_and_send',
    )(out_local, info, resid)


def attend_heads(q, k, v, seq_len, blk=128):
    n_tok, width = q.shape
    row = lax.broadcasted_iota(jnp.int32, (blk, blk), 0)
    col = lax.broadcasted_iota(jnp.int32, (blk, blk), 1)
    seen = (row >= col) & (row // seq_len == col // seq_len)
    heads = []
    for h in range(width // HEAD_DIM):
        tiles = []
        for t in range(n_tok // blk):
            at = (slice(t * blk, (t + 1) * blk), slice(h * HEAD_DIM, (h + 1) * HEAD_DIM))
            s = lax.dot_general(q[at], k[at], (((1,), (1,)), ((), ())), preferred_element_type=F32) * (HEAD_DIM ** -0.5)
            s = jnp.where(seen, s, -1e30)
            e = jnp.exp(s - jnp.max(s, axis=1, keepdims=True))
            p = (e / jnp.sum(e, axis=1, keepdims=True)).astype(BF16)
            tiles.append(jnp.dot(p, v[at], preferred_element_type=F32).astype(BF16))
        heads.append(jnp.concatenate(tiles, axis=0))
    return jnp.concatenate(heads, axis=1)


def qkv_kernel(n_blk, seq_len, y_ref, nw_ref, wq_ref, wk_ref, wv_ref, a_ref, x_scr, q_scr, k_scr, v_scr):
    i = pl.program_id(0)
    n_tok = y_ref.shape[0]
    rb = 16

    @pl.when(i == 0)
    def _():
        def norm(step, _):
            rows = pl.ds(pl.multiple_of(step * rb, rb), rb)
            y = y_ref[rows, :].astype(F32)
            inv = lax.rsqrt(jnp.mean(y * y, axis=1, keepdims=True) + NORM_EPS)
            x_scr[rows, :] = (y * inv * nw_ref[...]).astype(BF16)
            return 0

        lax.fori_loop(0, n_tok // rb, norm, 0)

    def attend():
        a_ref[...] = attend_heads(q_scr[...], k_scr[...], v_scr[...], seq_len)

    def project():
        q = jnp.dot(x_scr[...], wq_ref[...], preferred_element_type=F32).astype(BF16)
        k = jnp.dot(x_scr[...], wk_ref[...], preferred_element_type=F32).astype(BF16)
        v = jnp.dot(x_scr[...], wv_ref[...], preferred_element_type=F32).astype(BF16)
        q_scr[...] = q
        k_scr[...] = k
        v_scr[...] = v

    @pl.when(i == 0)
    def _():
        project()

    @pl.when((i > 0) & (i < n_blk))
    def _():
        attend()
        project()

    @pl.when(i == n_blk)
    def _():
        attend()


def qkv_attend(y, norm_w, w_q, w_k, w_v, seq_len, bn=256):
    n_tok, dim = y.shape
    width = w_q.shape[1]
    n_blk = width // bn
    w_spec = pl.BlockSpec((dim, bn), lambda i: (0, jnp.minimum(i, n_blk - 1)))
    return pl.pallas_call(
        functools.partial(qkv_kernel, n_blk, seq_len),
        grid=(n_blk + 1,),
        out_shape=jax.ShapeDtypeStruct((n_tok, width), BF16),
        in_specs=[pl.BlockSpec((n_tok, dim), lambda i: (0, 0), pipeline_mode=pl.Buffered(1)),
                  pl.BlockSpec((1, dim), lambda i: (0, 0), pipeline_mode=pl.Buffered(1)), w_spec, w_spec, w_spec],
        out_specs=pl.BlockSpec((n_tok, bn), lambda i: (0, jnp.maximum(i - 1, 0))),
        scratch_shapes=[pltpu.VMEM((n_tok, dim), BF16)] + [pltpu.VMEM((n_tok, bn), BF16)] * 3,
        compiler_params=pltpu.CompilerParams(dimension_semantics=('arbitrary',), vmem_limit_bytes=VMEM_LIMIT),
        name='qkv_attend',
    )(y, norm_w, w_q, w_k, w_v)


def out_kernel(seq_len, pos_ref, a_ref, y_ref, wo_ref, z_ref):
    proj = jnp.dot(a_ref[...], wo_ref[...], preferred_element_type=F32).astype(BF16)
    z = (y_ref[...].astype(F32) + proj.astype(F32)).astype(BF16)
    for s in range(z.shape[0] // seq_len):
        z_ref[pl.ds(pl.multiple_of(pos_ref[s] * seq_len, seq_len), seq_len), :] = z[s * seq_len:(s + 1) * seq_len]


def out_project(pos, a, y, w_o, seq_len, bn=256):
    n_tok, width = a.shape
    dim = w_o.shape[1]
    return pl.pallas_call(
        functools.partial(out_kernel, seq_len),
        grid_spec=pltpu.PrefetchScalarGridSpec(
            num_scalar_prefetch=1,
            grid=(dim // bn,),
            in_specs=[pl.BlockSpec((n_tok, width), lambda i, pos: (0, 0), pipeline_mode=pl.Buffered(1)),
                      pl.BlockSpec((n_tok, bn), lambda i, pos: (0, i)), pl.BlockSpec((width, bn), lambda i, pos: (0, i))],
            out_specs=pl.BlockSpec((n_tok, bn), lambda i, pos: (0, i)),
        ),
        out_shape=jax.ShapeDtypeStruct((n_tok, dim), BF16),
        compiler_params=pltpu.CompilerParams(dimension_semantics=('arbitrary',), vmem_limit_bytes=VMEM_LIMIT),
        name='out_project',
    )(pos, a, y, w_o)


def arrival_order(owner_row, n_ep):
    seq_dev = owner_row.shape[0] // n_ep
    grid = owner_row.reshape(n_ep, seq_dev)
    key = (grid // seq_dev) * seq_dev + jnp.arange(seq_dev)
    place = jnp.sum(key[:, None, :] < key[:, :, None], axis=2)
    chosen = (place[:, None, :] == jnp.arange(seq_dev)[:, None]).astype(jnp.int32)
    return jnp.sum(chosen * grid[:, None, :], axis=2), jnp.sum(chosen * jnp.arange(seq_dev), axis=2)


def solution(mesh):
    n_stages = mesh.shape['pp']
    n_ep = mesh.shape['ep']
    group_axes = ('data', 'pp')

    def device_step(expert_out, expert_id, slot_id, gate, resid, owner, norm_w, w_q, w_k, w_v, w_o):
        me = lax.axis_index('ep')
        out_local, h = expert_out[0, 0], resid[0, 0]
        n_exp, capacity, dim = out_local.shape
        cap_dev = capacity // n_ep
        n_tok = h.shape[0]
        n_seq = owner.shape[1]
        seq_dev = n_seq // n_ep
        seq_len = n_tok // seq_dev
        n_slot = n_exp * cap_dev

        owner_next = lax.ppermute(owner[0], 'pp', [((r + 1) % n_stages, r) for r in range(n_stages)])
        ids, slots = expert_id[0, 0], slot_id[0, 0]
        index = jnp.where(slots >= 0, ids * cap_dev + slots - me * cap_dev, -1).astype(F32)
        local = jnp.broadcast_to(jnp.arange(n_tok, dtype=F32)[:, None], (n_tok, 1))
        table = lax.all_gather(jnp.concatenate([index, gate[0, 0], local], axis=1), 'ep', axis=0, tiled=True)
        dest_seqs, _ = arrival_order(owner_next, n_ep)
        relative = jnp.bitwise_xor(me, jnp.array([0, 2, 1, 3]))
        pick = dest_seqs[relative].reshape(n_ep, n_ep, seq_dev // n_ep).transpose(1, 0, 2).reshape(n_seq)
        info = table.reshape(n_seq, seq_len * 17)[pick].reshape(n_ep, n_tok, 17)
        info = jnp.concatenate([info[:, :, :8] - (me * n_slot).astype(F32), info[:, :, 8:]], axis=2)

        y = combine_and_send(out_local, info, h, n_ep, n_stages)

        _, rows = arrival_order(owner[0], n_ep)
        pos = lax.dynamic_index_in_dim(rows, me, 0, keepdims=False).astype(jnp.int32)
        heads = qkv_attend(y, norm_w, w_q[0], w_k[0], w_v[0], seq_len)
        return out_project(pos, heads, y, w_o[0], seq_len)[None, None]

    tok_spec = P(group_axes, None, 'ep', None)
    weight_spec = P('pp', None, None)
    in_specs = (P(group_axes, None, 'ep', None, None), tok_spec, tok_spec, tok_spec, tok_spec, P(group_axes, None), P('pp', None), weight_spec,
                weight_spec, weight_spec, weight_spec)
    return jax.shard_map(device_step, mesh=mesh, in_specs=in_specs, out_specs=tok_spec, check_vma=False)
```

```python
import functools

import jax
import jax.numpy as jnp
from jax import lax
from jax.experimental import pallas as pl
from jax.experimental.pallas import tpu as pltpu
from jax.sharding import PartitionSpec as P

HEAD_DIM = 128
NORM_EPS = 1e-6
F32, BF16 = jnp.float32, jnp.bfloat16
MESH = pl.DeviceIdType.MESH
VMEM_LIMIT = 66_000_000


def stage_kernel(n_ep, n_stages, dk, bn, seq_len, o_hbm, info_ref, h_hbm, nw_ref, wq_hbm, wk_hbm, wv_hbm, wo_hbm, z_hbm, obuf, hbuf, w3, perm,
                 send_a, recv_a, keep, send_b, recv_b, send_c, y_own, xbuf, wbuf, abuf, q_scr, k_scr, v_scr, zscr, recv_z, zout,
                 o_sem, h_sem, sa_sem, ra_sem, sb_sem, rb_sem, sc_sem, rc_sem, sx_sem, rx_sem, w_sem, sz_sem, rz_sem, out_sem,
                 a_free, b_free, z_free):
    me = lax.axis_index('ep')
    rank = lax.axis_index('pp')
    core = lax.rem(me, 2)
    core_peer = me + 1 - 2 * core
    x_peer = lax.rem(me + 2, n_ep)
    next_rank = lax.rem(rank + 1, n_stages)
    prev_rank = lax.rem(rank + n_stages - 1, n_stages)
    n_exp, cap_dev, n_slot = obuf.shape[1], obuf.shape[2], perm.shape[1] * 3
    n_tok, dim = h_hbm.shape
    n_slot = n_exp * cap_dev
    rows_g = n_tok // 2
    sub = rows_g // n_ep
    nk = dim // dk
    n_unit = 2 * nk
    ring_a, ring_b, ring_c = recv_a.shape[0], keep.shape[0], send_c.shape[0]
    width = abuf.shape[1]
    n_hp = width // bn
    n_ot = dim // bn
    n_w, ring_z, ring_r = wbuf.shape[0], zscr.shape[0], recv_z.shape[0]
    n_tile = 3 * n_hp + n_ot

    def col(k, w):
        return pl.ds(pl.multiple_of(k * w, w), w)

    def o_copy(u, o):
        j = lax.rem(me + o, n_ep)
        return pltpu.make_async_copy(o_hbm.at[:, col(j, cap_dev), col(lax.rem(u, nk), dk)], obuf.at[o], o_sem.at[o])

    def h_copy(u):
        return pltpu.make_async_copy(h_hbm.at[:, col(lax.rem(u, nk), dk)], hbuf, h_sem.at[0])

    def to_core(src, dst, s_sem, r_sem):
        return pltpu.make_async_remote_copy(src, dst, s_sem, r_sem, device_id={'ep': core_peer}, device_id_type=MESH)

    def a_copy(u):
        return to_core(send_a.at[lax.rem(u, 2)], recv_a.at[lax.rem(u, ring_a)], sa_sem.at[lax.rem(u, 2)], ra_sem.at[lax.rem(u, ring_a)])

    def b_copy(u):
        i = lax.rem(u, ring_b)
        return pltpu.make_async_remote_copy(send_b.at[i], recv_b.at[i], sb_sem.at[i], rb_sem.at[i], device_id={'ep': x_peer}, device_id_type=MESH)

    def c_copy(u):
        i = lax.rem(u, ring_c)
        return pltpu.make_async_remote_copy(send_c.at[i], y_own.at[u // nk, :, col(lax.rem(u, nk), dk)], sc_sem.at[i], rc_sem.at[u],
                                            device_id={'pp': next_rank}, device_id_type=MESH)

    def x_copy(g, p):
        at = xbuf.at[g, pl.ds(pl.multiple_of(core * rows_g + p * 32, 32), 32)]
        return to_core(at, at, sx_sem.at[p], rx_sem.at[g * (rows_g // 32) + p])

    def z_copy(t):
        theirs = pl.ds(pl.multiple_of((1 - core) * rows_g, rows_g), rows_g)
        return to_core(zscr.at[lax.rem(t, ring_z), theirs], recv_z.at[lax.rem(t, ring_r)], sz_sem.at[lax.rem(t, ring_z)], rz_sem.at[lax.rem(t, ring_r)])

    def out_copy(t):
        i = lax.rem(t, ring_z)
        return pltpu.make_async_copy(zout.at[i], z_hbm.at[col(t // n_ot, rows_g), col(lax.rem(t, n_ot), bn)], out_sem.at[i])

    def w_slot(s):
        return wbuf.at[lax.rem(s, n_w)], w_sem.at[lax.rem(s, n_w)]

    def qkv_tile(s, hp, kind):
        slot, sem = w_slot(s)
        return pltpu.make_async_copy((wq_hbm, wk_hbm, wv_hbm)[kind].at[:, col(core * n_hp + hp, bn)], slot, sem)

    def out_tile(s, t):
        slot, sem = w_slot(s)
        return pltpu.make_async_copy(wo_hbm.at[col(core, width), col(t, bn)], slot.at[pl.ds(0, width)], sem)

    def start_tile(s):
        at = lax.rem(s, n_tile)

        @pl.when(s < 2 * n_tile)
        def _():
            for kind in range(3):
                @pl.when((at < 3 * n_hp) & (lax.rem(at, 3) == kind))
                def _():
                    qkv_tile(s, at // 3, kind).start()

            @pl.when(at >= 3 * n_hp)
            def _():
                out_tile(s, at - 3 * n_hp).start()

    for o in range(n_ep):
        o_copy(0, o).start()
    h_copy(0).start()
    for s in range(n_w):
        qkv_tile(s, s // 3, s % 3).start()

    barrier = pltpu.get_barrier_semaphore()
    pl.semaphore_signal(barrier, inc=1, device_id={'ep': core_peer}, device_id_type=MESH)
    pl.semaphore_signal(barrier, inc=1, device_id={'ep': x_peer}, device_id_type=MESH)
    pl.semaphore_signal(barrier, inc=1, device_id={'pp': prev_rank}, device_id_type=MESH)

    def build(g):
        def block(step, _):
            o = step // n_ep
            part = lax.rem(step, n_ep) * sub
            rows = info_ref[lax.rem(me + o, n_ep), pl.ds(pl.multiple_of(g * rows_g + part, sub), sub), :]
            slot = lax.broadcasted_iota(jnp.int32, (sub, n_slot), 1).astype(F32)
            w = jnp.zeros((sub, n_slot), F32)
            for c in range(8):
                w = jnp.where(rows[:, c:c + 1] == slot, rows[:, 8 + c:9 + c], w)
            for t in range(3):
                high = w.astype(BF16)
                w3[o, pl.ds(pl.multiple_of(t * rows_g + part, sub), sub), :] = high
                w = w - high.astype(F32)
            return 0

        lax.fori_loop(0, n_ep * n_ep, block, 0)
        home = info_ref[me, pl.ds(pl.multiple_of(g * rows_g, rows_g), rows_g), 16:17]
        perm[...] = (home == lax.broadcasted_iota(jnp.int32, (rows_g, n_tok), 1).astype(F32)).astype(F32).astype(BF16)

    def partial_sums(u):
        @pl.when(lax.rem(u, nk) == 0)
        def _():
            build(u // nk)

        @pl.when(u >= 2)
        def _():
            a_copy(u - 2).wait_send()

        @pl.when(u >= ring_b)
        def _():
            b_copy(u - ring_b).wait_send()

        for o in range(n_ep):
            o_copy(u, o).wait()
            rows = obuf[o].reshape(n_slot, dk)
            split = jnp.dot(w3[o], rows, preferred_element_type=F32)
            part = split[:rows_g] + split[rows_g:2 * rows_g] + split[2 * rows_g:]
            if o == 0:
                h_copy(u).wait()
                part += jnp.dot(perm[...], hbuf[...], preferred_element_type=F32)
            place = pl.ds(pl.multiple_of(lax.rem(me + o, n_ep) * sub, sub), sub)
            keep[lax.rem(u, ring_b), place, :] = part[0:sub]
            send_b[lax.rem(u, ring_b), place, :] = part[sub:2 * sub]
            send_a[lax.rem(u, 2), 0, place, :] = part[2 * sub:3 * sub]
            send_a[lax.rem(u, 2), 1, place, :] = part[3 * sub:4 * sub]

            @pl.when(u + 1 < n_unit)
            def _():
                o_copy(u + 1, o).start()
                if o == 0:
                    h_copy(u + 1).start()

        @pl.when(u >= ring_a)
        def _():
            pl.semaphore_wait(a_free, 1)

        a_copy(u).start()

    def across_x(u):
        i = lax.rem(u, ring_b)
        a_copy(u).wait_recv()
        keep[i] = keep[i] + recv_a[lax.rem(u, ring_a), 0]
        send_b[i] = send_b[i] + recv_a[lax.rem(u, ring_a), 1]

        @pl.when(u < n_unit - ring_a)
        def _():
            pl.semaphore_signal(a_free, inc=1, device_id={'ep': core_peer}, device_id_type=MESH)

        @pl.when(u >= ring_b)
        def _():
            pl.semaphore_wait(b_free, 1)

        b_copy(u).start()

    def across_y(u):
        i = lax.rem(u, ring_b)
        b_copy(u).wait_recv()

        @pl.when(u >= ring_c)
        def _():
            c_copy(u - ring_c).wait_send()

        send_c[lax.rem(u, ring_c)] = (keep[i] + recv_b[i]).astype(BF16)
        c_copy(u).start()

        @pl.when(u < n_unit - ring_b)
        def _():
            pl.semaphore_signal(b_free, inc=1, device_id={'ep': x_peer}, device_id_type=MESH)

    pl.semaphore_wait(barrier, 3)
    ahead = nk - 2

    def phase_one(u, _):
        @pl.when(u < n_unit)
        def _():
            partial_sums(u)

        @pl.when(u >= 1)
        def _():
            across_x(u - 1)

        @pl.when((u >= 4) & (lax.rem(u, 2) == 0) & (u // 2 - 2 < ahead))
        def _():
            across_y(u // 2 - 2)

        return 0

    lax.fori_loop(0, n_unit + 1, phase_one, 0)

    def attend(hp):
        abuf[:, col(hp, bn)] = attend_heads(q_scr[...], k_scr[...], v_scr[...], seq_len)

    q_scr[...] = jnp.zeros_like(q_scr)
    k_scr[...] = jnp.zeros_like(k_scr)
    v_scr[...] = jnp.zeros_like(v_scr)
    n_under = n_hp // 2
    n_last = 3

    def finish(t):
        g, i = t // n_ot, lax.rem(t, ring_z)
        mine = pl.ds(pl.multiple_of(core * rows_g, rows_g), rows_g)
        z_copy(t).wait_recv()
        proj = (zscr[i, mine, :] + recv_z[lax.rem(t, ring_r)]).astype(BF16)

        @pl.when(t < 2 * n_ot - ring_r)
        def _():
            pl.semaphore_signal(z_free, inc=1, device_id={'ep': core_peer}, device_id_type=MESH)

        @pl.when(t >= ring_z)
        def _():
            out_copy(t - ring_z).wait()

        zout[i] = (y_own[g, :, col(lax.rem(t, n_ot), bn)].astype(F32) + proj.astype(F32)).astype(BF16)
        out_copy(t).start()

    def group_pass(g, _):
        def late(u, _):
            across_y(u)
            return 0

        lax.fori_loop(jnp.where(g == 0, ahead, n_unit - n_last), jnp.where(g == 0, nk, n_unit), late, 0)

        def arrived(k, _):
            c_copy(g * nk + k).wait_recv()
            return 0

        lax.fori_loop(0, nk, arrived, 0)

        def norm(p, _):
            for half in range(2):
                y = y_own[g, pl.ds(pl.multiple_of(p * 32 + half * 16, 16), 16), :].astype(F32)
                inv = lax.rsqrt(jnp.mean(y * y, axis=1, keepdims=True) + NORM_EPS)
                xbuf[g, pl.ds(pl.multiple_of(core * rows_g + p * 32 + half * 16, 16), 16), :] = (y * inv * nw_ref[...]).astype(BF16)
            x_copy(g, p).start()
            return 0

        lax.fori_loop(0, rows_g // 32, norm, 0)

        def exchanged(p, _):
            x_copy(g, p).wait()
            return 0

        lax.fori_loop(0, rows_g // 32, exchanged, 0)

        def heads(hp, _):
            s = g * n_tile + hp * 3
            for kind in range(3):
                qkv_tile(s + kind, hp, kind).wait()
            attend(jnp.maximum(hp - 1, 0))
            q = jnp.dot(xbuf[g], wbuf[lax.rem(s, n_w)], preferred_element_type=F32).astype(BF16)
            k = jnp.dot(xbuf[g], wbuf[lax.rem(s + 1, n_w)], preferred_element_type=F32).astype(BF16)
            v = jnp.dot(xbuf[g], wbuf[lax.rem(s + 2, n_w)], preferred_element_type=F32).astype(BF16)
            q_scr[...] = q
            k_scr[...] = k
            v_scr[...] = v
            for kind in range(3):
                start_tile(s + kind + n_w)

            @pl.when((g == 0) & (lax.rem(hp, 2) == 1))
            def _():
                across_y(nk + hp // 2)

            return 0

        lax.fori_loop(0, n_hp, heads, 0)
        attend(n_hp - 1)

        def project(i, _):
            for r in range(2):
                t = g * n_ot + 2 * i + r
                s = g * n_tile + 3 * n_hp + 2 * i + r

                @pl.when(t >= ring_z)
                def _():
                    z_copy(t - ring_z).wait_send()

                out_tile(s, 2 * i + r).wait()
            for r in range(2):
                t = g * n_ot + 2 * i + r
                s = g * n_tile + 3 * n_hp + 2 * i + r
                zscr[lax.rem(t, ring_z)] = jnp.dot(abuf[...], wbuf[lax.rem(s, n_w), 0:width, :], preferred_element_type=F32)
            for r in range(2):
                t = g * n_ot + 2 * i + r
                start_tile(g * n_tile + 3 * n_hp + 2 * i + r + n_w)

                @pl.when(t >= ring_r)
                def _():
                    pl.semaphore_wait(z_free, 1)

                z_copy(t).start()

            @pl.when(i >= 1)
            def _():
                finish(g * n_ot + 2 * i - 2)
                finish(g * n_ot + 2 * i - 1)

            @pl.when((g == 0) & (lax.rem(i, 5) == 2))
            def _():
                across_y(nk + n_under + i // 5)

            return 0

        lax.fori_loop(0, n_ot // 2, project, 0)
        finish(g * n_ot + n_ot - 2)
        finish(g * n_ot + n_ot - 1)
        return 0

    lax.fori_loop(0, 2, group_pass, 0)

    for u in range(n_unit - 2, n_unit):
        a_copy(u).wait_send()
    for u in range(n_unit - ring_b, n_unit):
        b_copy(u).wait_send()
    for u in range(n_unit - ring_c, n_unit):
        c_copy(u).wait_send()
    for t in range(2 * n_ot - ring_z, 2 * n_ot):
        z_copy(t).wait_send()
        out_copy(t).wait()


def stage(out_local, info, resid, norm_w, w_q, w_k, w_v, w_o, seq_len, n_ep, n_stages, dk=512, bn=256):
    n_exp, capacity, dim = out_local.shape
    n_tok = resid.shape[0]
    cap_dev = capacity // n_ep
    n_slot = n_exp * cap_dev
    width = w_q.shape[1] // 2
    rows_g = n_tok // 2
    n_unit = 2 * dim // dk
    n_w, ring_a, ring_b, ring_c, ring_z, ring_r = 6, 4, 16, 4, 4, 8
    any_spec = pl.BlockSpec(memory_space=pl.ANY)
    vmem_spec = pl.BlockSpec(memory_space=pltpu.VMEM)
    vmem, dma = pltpu.VMEM, pltpu.SemaphoreType.DMA
    return pl.pallas_call(
        functools.partial(stage_kernel, n_ep, n_stages, dk, bn, seq_len),
        out_shape=jax.ShapeDtypeStruct((n_tok, dim), BF16),
        in_specs=[any_spec, vmem_spec, any_spec, vmem_spec] + [any_spec] * 4,
        out_specs=any_spec,
        scratch_shapes=[
            vmem((n_ep, n_exp, cap_dev, dk), BF16),
            vmem((n_tok, dk), BF16),
            vmem((n_ep, 3 * rows_g, n_slot), BF16),
            vmem((rows_g, n_tok), BF16),
            vmem((2, 2, rows_g, dk), F32),
            vmem((ring_a, 2, rows_g, dk), F32),
            vmem((ring_b, rows_g, dk), F32),
            vmem((ring_b, rows_g, dk), F32),
            vmem((ring_b, rows_g, dk), F32),
            vmem((ring_c, rows_g, dk), BF16),
            vmem((2, rows_g, dim), BF16),
            vmem((2, n_tok, dim), BF16),
            vmem((n_w, dim, bn), BF16),
            vmem((n_tok, width), BF16),
            vmem((n_tok, bn), BF16), vmem((n_tok, bn), BF16), vmem((n_tok, bn), BF16),
            vmem((ring_z, n_tok, bn), F32),
            vmem((ring_r, rows_g, bn), F32),
            vmem((ring_z, rows_g, bn), BF16),
            dma((n_ep,)), dma((1,)), dma((2,)), dma((ring_a,)), dma((ring_b,)), dma((ring_b,)), dma((ring_c,)), dma((n_unit,)),
            dma((rows_g // 32,)), dma((2 * rows_g // 32,)), dma((n_w,)), dma((ring_z,)), dma((ring_r,)), dma((ring_z,)),
            pltpu.SemaphoreType.REGULAR, pltpu.SemaphoreType.REGULAR, pltpu.SemaphoreType.REGULAR,
        ],
        compiler_params=pltpu.CompilerParams(collective_id=0, has_side_effects=True, vmem_limit_bytes=VMEM_LIMIT),
        name='stage',
    )(out_local, info, resid, norm_w, w_q, w_k, w_v, w_o)


def attend_heads(q, k, v, seq_len, blk=128):
    n_tok, width = q.shape
    row = lax.broadcasted_iota(jnp.int32, (blk, blk), 0)
    col = lax.broadcasted_iota(jnp.int32, (blk, blk), 1)
    seen = (row >= col) & (row // seq_len == col // seq_len)
    heads = []
    for h in range(width // HEAD_DIM):
        tiles = []
        for t in range(n_tok // blk):
            at = (slice(t * blk, (t + 1) * blk), slice(h * HEAD_DIM, (h + 1) * HEAD_DIM))
            s = lax.dot_general(q[at], k[at], (((1,), (1,)), ((), ())), preferred_element_type=F32) * (HEAD_DIM ** -0.5)
            s = jnp.where(seen, s, -1e30)
            e = jnp.exp(s - jnp.max(s, axis=1, keepdims=True))
            p = (e / jnp.sum(e, axis=1, keepdims=True)).astype(BF16)
            tiles.append(jnp.dot(p, v[at], preferred_element_type=F32).astype(BF16))
        heads.append(jnp.concatenate(tiles, axis=0))
    return jnp.concatenate(heads, axis=1)


def place_kernel(src_ref, z_ref, out_ref):
    out_ref[...] = z_ref[...]


def place_sequences(src, z, seq_len):
    n_tok, dim = z.shape
    return pl.pallas_call(
        place_kernel,
        grid_spec=pltpu.PrefetchScalarGridSpec(
            num_scalar_prefetch=1,
            grid=(n_tok // seq_len,),
            in_specs=[pl.BlockSpec((seq_len, dim), lambda i, src: (src[i], 0))],
            out_specs=pl.BlockSpec((seq_len, dim), lambda i, src: (i, 0)),
        ),
        out_shape=jax.ShapeDtypeStruct((n_tok, dim), BF16),
        compiler_params=pltpu.CompilerParams(dimension_semantics=('arbitrary',)),
        name='place_sequences',
    )(src, z)


def arrival_order(owner_row, n_ep):
    seq_dev = owner_row.shape[0] // n_ep
    grid = owner_row.reshape(n_ep, seq_dev)
    key = (grid // seq_dev) * seq_dev + jnp.arange(seq_dev)
    place = jnp.sum(key[:, None, :] < key[:, :, None], axis=2)
    chosen = (place[:, None, :] == jnp.arange(seq_dev)[:, None]).astype(jnp.int32)
    return jnp.sum(chosen * grid[:, None, :], axis=2), place


def solution(mesh):
    n_stages = mesh.shape['pp']
    n_ep = mesh.shape['ep']
    group_axes = ('data', 'pp')

    def device_step(expert_out, expert_id, slot_id, gate, resid, owner, norm_w, w_q, w_k, w_v, w_o):
        me = lax.axis_index('ep')
        out_local, h = expert_out[0, 0], resid[0, 0]
        n_exp, capacity, dim = out_local.shape
        cap_dev = capacity // n_ep
        n_tok = h.shape[0]
        n_seq = owner.shape[1]
        seq_dev = n_seq // n_ep
        seq_len = n_tok // seq_dev
        n_slot = n_exp * cap_dev

        owner_next = lax.ppermute(owner[0], 'pp', [((r + 1) % n_stages, r) for r in range(n_stages)])
        ids, slots = expert_id[0, 0], slot_id[0, 0]
        index = jnp.where(slots >= 0, ids * cap_dev + slots - me * cap_dev, -1).astype(F32)
        local = jnp.broadcast_to(jnp.arange(n_tok, dtype=F32)[:, None], (n_tok, 1))
        table = lax.all_gather(jnp.concatenate([index, gate[0, 0], local], axis=1), 'ep', axis=0, tiled=True)
        dest_seqs, _ = arrival_order(owner_next, n_ep)
        relative = jnp.bitwise_xor(me, jnp.array([0, 2, 1, 3]))
        pick = dest_seqs[relative].reshape(n_ep, n_ep, seq_dev // n_ep).transpose(1, 2, 0).reshape(n_seq)
        info = table.reshape(n_seq, seq_len * 17)[pick].reshape(n_ep, n_tok, 17)
        info = jnp.concatenate([info[:, :, :8] - (me * n_slot).astype(F32), info[:, :, 8:]], axis=2)

        z = stage(out_local, info, h, norm_w, w_q[0], w_k[0], w_v[0], w_o[0], seq_len, n_ep, n_stages)

        _, places = arrival_order(owner[0], n_ep)
        place = lax.dynamic_index_in_dim(places, me, 0, keepdims=False)
        src = (place % 2 * n_ep + place // 2).astype(jnp.int32)
        return place_sequences(src, z, seq_len)[None, None]

    tok_spec = P(group_axes, None, 'ep', None)
    weight_spec = P('pp', None, None)
    in_specs = (P(group_axes, None, 'ep', None, None), tok_spec, tok_spec, tok_spec, tok_spec, P(group_axes, None), P('pp', None), weight_spec,
                weight_spec, weight_spec, weight_spec)
    return jax.shard_map(device_step, mesh=mesh, in_specs=in_specs, out_specs=tok_spec, check_vma=False)
```

```python
import functools

import jax
import jax.numpy as jnp
from jax import lax
from jax.experimental import pallas as pl
from jax.experimental.pallas import tpu as pltpu
from jax.sharding import PartitionSpec as P

HEAD_DIM = 128
NORM_EPS = 1e-6
F32, BF16 = jnp.float32, jnp.bfloat16
MESH = pl.DeviceIdType.MESH
VMEM_LIMIT = 66_000_000


def stage_kernel(n_ep, n_stages, dk, bn, seq_len, o_hbm, table_ref, meta_ref, h_hbm, nw_ref, wq_hbm, wk_hbm, wv_hbm, wo_hbm, z_hbm, tables, meta, obuf, hbuf, w3, perm,
                 send_a, recv_a, keep, send_b, recv_b, send_c, y_own, xbuf, wbuf, abuf, q_scr, k_scr, v_scr, zscr, recv_z, zout,
                 o_sem, h_sem, sa_sem, ra_sem, sb_sem, rb_sem, sc_sem, rc_sem, sx_sem, rx_sem, w_sem, sz_sem, rz_sem, out_sem,
                 st_sem, rt_sem, sm_sem, rm_sem, a_free, b_free, z_free):
    me = lax.axis_index('ep')
    rank = lax.axis_index('pp')
    core = lax.rem(me, 2)
    core_peer = me + 1 - 2 * core
    x_peer = lax.rem(me + 2, n_ep)
    other_rank = 1 - rank
    n_exp, cap_dev, n_slot = obuf.shape[1], obuf.shape[2], perm.shape[1] * 3
    n_tok, dim = h_hbm.shape
    n_slot = n_exp * cap_dev
    rows_g = n_tok // 2
    sub = rows_g // n_ep
    nk = dim // dk
    n_unit = 2 * nk
    ring_a, ring_b, ring_c = recv_a.shape[0], keep.shape[0], send_c.shape[0]
    width = abuf.shape[1]
    n_hp = width // bn
    n_ot = dim // bn
    n_w, ring_z, ring_r = wbuf.shape[0], zscr.shape[0], recv_z.shape[0]
    n_tile = 3 * n_hp + n_ot

    def col(k, w):
        return pl.ds(pl.multiple_of(k * w, w), w)

    def o_copy(u, o):
        j = lax.rem(me + o, n_ep)
        return pltpu.make_async_copy(o_hbm.at[:, col(j, cap_dev), col(lax.rem(u, nk), dk)], obuf.at[o], o_sem.at[o])

    def h_copy(u):
        return pltpu.make_async_copy(h_hbm.at[:, col(lax.rem(u, nk), dk)], hbuf, h_sem.at[0])

    def to_core(src, dst, s_sem, r_sem):
        return pltpu.make_async_remote_copy(src, dst, s_sem, r_sem, device_id={'ep': core_peer}, device_id_type=MESH)

    def a_copy(u):
        return to_core(send_a.at[lax.rem(u, 2)], recv_a.at[lax.rem(u, ring_a)], sa_sem.at[lax.rem(u, 2)], ra_sem.at[lax.rem(u, ring_a)])

    def b_copy(u):
        i = lax.rem(u, ring_b)
        return pltpu.make_async_remote_copy(send_b.at[i], recv_b.at[i], sb_sem.at[i], rb_sem.at[i], device_id={'ep': x_peer}, device_id_type=MESH)

    def c_copy(u):
        i = lax.rem(u, ring_c)
        return pltpu.make_async_remote_copy(send_c.at[i], y_own.at[u // nk, :, col(lax.rem(u, nk), dk)], sc_sem.at[i], rc_sem.at[u],
                                            device_id={'pp': other_rank}, device_id_type=MESH)

    def x_copy(g, p):
        at = xbuf.at[g, pl.ds(pl.multiple_of(core * rows_g + p * 32, 32), 32)]
        return to_core(at, at, sx_sem.at[p], rx_sem.at[g * (rows_g // 32) + p])

    def z_copy(t):
        theirs = pl.ds(pl.multiple_of((1 - core) * rows_g, rows_g), rows_g)
        return to_core(zscr.at[lax.rem(t, ring_z), theirs], recv_z.at[lax.rem(t, ring_r)], sz_sem.at[lax.rem(t, ring_z)], rz_sem.at[lax.rem(t, ring_r)])

    def out_copy(t):
        i = lax.rem(t, ring_z)
        return pltpu.make_async_copy(zout.at[i], z_hbm.at[col(t // n_ot, rows_g), col(lax.rem(t, n_ot), bn)], out_sem.at[i])

    def w_slot(s):
        return wbuf.at[lax.rem(s, n_w)], w_sem.at[lax.rem(s, n_w)]

    def qkv_tile(s, hp, kind):
        slot, sem = w_slot(s)
        return pltpu.make_async_copy((wq_hbm, wk_hbm, wv_hbm)[kind].at[:, col(core * n_hp + hp, bn)], slot, sem)

    def out_tile(s, t):
        slot, sem = w_slot(s)
        return pltpu.make_async_copy(wo_hbm.at[col(core, width), col(t, bn)], slot.at[pl.ds(0, width)], sem)

    def start_tile(s):
        at = lax.rem(s, n_tile)

        @pl.when(s < 2 * n_tile)
        def _():
            for kind in range(3):
                @pl.when((at < 3 * n_hp) & (lax.rem(at, 3) == kind))
                def _():
                    qkv_tile(s, at // 3, kind).start()

            @pl.when(at >= 3 * n_hp)
            def _():
                out_tile(s, at - 3 * n_hp).start()

    for o in range(n_ep):
        o_copy(0, o).start()
    h_copy(0).start()
    barrier = pltpu.get_barrier_semaphore()
    for o in range(1, n_ep):
        pl.semaphore_signal(barrier, inc=1, device_id={'ep': lax.rem(me + o, n_ep)}, device_id_type=MESH)
    pl.semaphore_signal(barrier, inc=1, device_id={'pp': other_rank}, device_id_type=MESH)

    def table_copy(o, source):
        return pltpu.make_async_remote_copy(table_ref, tables.at[source], st_sem.at[o], rt_sem.at[source],
                                            device_id={'ep': lax.rem(me + o, n_ep)}, device_id_type=MESH)

    meta_copy = pltpu.make_async_remote_copy(meta_ref, meta, sm_sem.at[0], rm_sem.at[0], device_id={'pp': other_rank}, device_id_type=MESH)

    def build(g):
        slot = lax.broadcasted_iota(jnp.int32, (sub, n_slot), 1).astype(F32) + (me * n_slot).astype(F32)
        token = lax.broadcasted_iota(jnp.int32, (sub, n_tok), 1).astype(F32)
        line = lax.broadcasted_iota(jnp.int32, (sub, 1), 0).astype(F32)

        def block(o, _):
            j = lax.rem(me + o, n_ep)
            table = tables[j].T
            code = meta[pl.ds(j, 1), :]
            for r in range(n_ep):
                dest = 2 * (me // 2) + core if r == 0 else 2 * (1 - me // 2) + core if r == 1 else 2 * (me // 2) + 1 - core if r == 2 else 2 * (1 - me // 2) + 1 - core
                want = (2 * dest + g).astype(F32)
                rows = jnp.zeros((sub, table.shape[1]), F32)
                home = jnp.zeros((1, 1), F32)
                for q in range(n_tok // sub):
                    here = code[:, q:q + 1] == want
                    rows = jnp.where(here, table[q * sub:(q + 1) * sub], rows)
                    home = jnp.where(here, float(q * sub), home)
                w = jnp.zeros((sub, n_slot), F32)
                for c in range(8):
                    w = jnp.where(rows[:, c:c + 1] == slot, rows[:, 8 + c:9 + c], w)
                for t in range(3):
                    high = w.astype(BF16)
                    w3[o, t * rows_g + r * sub:t * rows_g + (r + 1) * sub, :] = high
                    w = w - high.astype(F32)

                @pl.when(o == 0)
                def _():
                    perm[r * sub:(r + 1) * sub, :] = (home + line == token).astype(F32).astype(BF16)

            return 0

        lax.fori_loop(0, n_ep, block, 0)

    def partial_sums(u):
        @pl.when(lax.rem(u, nk) == 0)
        def _():
            build(u // nk)

        @pl.when(u >= 2)
        def _():
            a_copy(u - 2).wait_send()

        @pl.when(u >= ring_b)
        def _():
            b_copy(u - ring_b).wait_send()

        for o in range(n_ep):
            o_copy(u, o).wait()
            rows = obuf[o].reshape(n_slot, dk)
            split = jnp.dot(w3[o], rows, preferred_element_type=F32)
            part = split[:rows_g] + split[rows_g:2 * rows_g] + split[2 * rows_g:]
            if o == 0:
                h_copy(u).wait()
                part += jnp.dot(perm[...], hbuf[...], preferred_element_type=F32)
            place = pl.ds(pl.multiple_of(lax.rem(me + o, n_ep) * sub, sub), sub)
            keep[lax.rem(u, ring_b), place, :] = part[0:sub]
            send_b[lax.rem(u, ring_b), place, :] = part[sub:2 * sub]
            send_a[lax.rem(u, 2), 0, place, :] = part[2 * sub:3 * sub]
            send_a[lax.rem(u, 2), 1, place, :] = part[3 * sub:4 * sub]

            @pl.when(u + 1 < n_unit)
            def _():
                o_copy(u + 1, o).start()
                if o == 0:
                    h_copy(u + 1).start()

        @pl.when(u >= ring_a)
        def _():
            pl.semaphore_wait(a_free, 1)

        a_copy(u).start()

    def across_x(u):
        i = lax.rem(u, ring_b)
        a_copy(u).wait_recv()
        keep[i] = keep[i] + recv_a[lax.rem(u, ring_a), 0]
        send_b[i] = send_b[i] + recv_a[lax.rem(u, ring_a), 1]

        @pl.when(u < n_unit - ring_a)
        def _():
            pl.semaphore_signal(a_free, inc=1, device_id={'ep': core_peer}, device_id_type=MESH)

        @pl.when(u >= ring_b)
        def _():
            pl.semaphore_wait(b_free, 1)

        b_copy(u).start()

    def across_y(u):
        i = lax.rem(u, ring_b)
        b_copy(u).wait_recv()

        @pl.when(u >= ring_c)
        def _():
            c_copy(u - ring_c).wait_send()

        send_c[lax.rem(u, ring_c)] = (keep[i] + recv_b[i]).astype(BF16)
        c_copy(u).start()

        @pl.when(u < n_unit - ring_b)
        def _():
            pl.semaphore_signal(b_free, inc=1, device_id={'ep': x_peer}, device_id_type=MESH)

    pl.semaphore_wait(barrier, n_ep)
    meta_copy.start()
    for o in range(1, n_ep):
        table_copy(o, me).start()
    tables[me] = table_ref[...]
    meta_copy.wait_recv()
    for o in range(1, n_ep):
        table_copy(o, lax.rem(me + o, n_ep)).wait_recv()
    ahead = nk - 2

    def phase_one(u, _):
        @pl.when(u < n_unit)
        def _():
            partial_sums(u)

        @pl.when((u >= 2) & (u < 2 + n_w))
        def _():
            start_tile(u - 2)

        @pl.when(u >= 1)
        def _():
            across_x(u - 1)

        @pl.when((u >= 4) & (lax.rem(u, 2) == 0) & (u // 2 - 2 < ahead))
        def _():
            across_y(u // 2 - 2)

        return 0

    lax.fori_loop(0, n_unit + 1, phase_one, 0)

    def attend(hp):
        abuf[:, col(hp, bn)] = head_mix(head_probs(head_scores(q_scr[...], k_scr[...]), seq_len), v_scr[...])

    q_scr[...] = jnp.zeros_like(q_scr)
    k_scr[...] = jnp.zeros_like(k_scr)
    v_scr[...] = jnp.zeros_like(v_scr)

    def under(hp):
        return (hp + 1) * 3 // 5 if isinstance(hp, int) else lax.div((hp + 1) * 3, 5)

    n_last = max(0, nk - under(n_hp - 1) - (n_ot // 2 + 2) // 3)

    def finish(t):
        g, i = t // n_ot, lax.rem(t, ring_z)
        mine = pl.ds(pl.multiple_of(core * rows_g, rows_g), rows_g)
        z_copy(t).wait_recv()
        proj = (zscr[i, mine, :] + recv_z[lax.rem(t, ring_r)]).astype(BF16)

        @pl.when(t < 2 * n_ot - ring_r)
        def _():
            pl.semaphore_signal(z_free, inc=1, device_id={'ep': core_peer}, device_id_type=MESH)

        @pl.when(t >= ring_z)
        def _():
            out_copy(t - ring_z).wait()

        zout[i] = (y_own[g, :, col(lax.rem(t, n_ot), bn)].astype(F32) + proj.astype(F32)).astype(BF16)
        out_copy(t).start()

    def group_pass(g, _):
        def late(u, _):
            across_y(u)
            return 0

        lax.fori_loop(jnp.where(g == 0, ahead, n_unit - n_last), jnp.where(g == 0, nk, n_unit), late, 0)

        def arrived(k, _):
            c_copy(g * nk + k).wait_recv()
            return 0

        lax.fori_loop(0, nk, arrived, 0)

        def norm(p, _):
            for half in range(2):
                y = y_own[g, pl.ds(pl.multiple_of(p * 32 + half * 16, 16), 16), :].astype(F32)
                inv = lax.rsqrt(jnp.mean(y * y, axis=1, keepdims=True) + NORM_EPS)
                xbuf[g, pl.ds(pl.multiple_of(core * rows_g + p * 32 + half * 16, 16), 16), :] = (y * inv * nw_ref[...]).astype(BF16)
            x_copy(g, p).start()
            return 0

        lax.fori_loop(0, rows_g // 32, norm, 0)

        def exchanged(p, _):
            x_copy(g, p).wait()
            return 0

        lax.fori_loop(0, rows_g // 32, exchanged, 0)

        def heads(hp, _):
            s = g * n_tile + hp * 3
            for kind in range(3):
                qkv_tile(s + kind, hp, kind).wait()
            scores = head_scores(q_scr[...], k_scr[...])
            q = jnp.dot(xbuf[g], wbuf[lax.rem(s, n_w)], preferred_element_type=F32).astype(BF16)
            mixed = head_mix(head_probs(scores, seq_len), v_scr[...])
            k = jnp.dot(xbuf[g], wbuf[lax.rem(s + 1, n_w)], preferred_element_type=F32).astype(BF16)
            v = jnp.dot(xbuf[g], wbuf[lax.rem(s + 2, n_w)], preferred_element_type=F32).astype(BF16)
            abuf[:, col(jnp.maximum(hp - 1, 0), bn)] = mixed
            q_scr[...] = q
            k_scr[...] = k
            v_scr[...] = v
            for kind in range(3):
                start_tile(s + kind + n_w)

            @pl.when((g == 0) & (under(hp) > under(hp - 1)))
            def _():
                across_y(nk + under(hp) - 1)

            return 0

        lax.fori_loop(0, n_hp, heads, 0)
        attend(n_hp - 1)

        def project(i, _):
            for r in range(2):
                t = g * n_ot + 2 * i + r
                s = g * n_tile + 3 * n_hp + 2 * i + r

                @pl.when(t >= ring_z)
                def _():
                    z_copy(t - ring_z).wait_send()

                out_tile(s, 2 * i + r).wait()
            for r in range(2):
                t = g * n_ot + 2 * i + r
                s = g * n_tile + 3 * n_hp + 2 * i + r
                zscr[lax.rem(t, ring_z)] = jnp.dot(abuf[...], wbuf[lax.rem(s, n_w), 0:width, :], preferred_element_type=F32)
            for r in range(2):
                t = g * n_ot + 2 * i + r
                start_tile(g * n_tile + 3 * n_hp + 2 * i + r + n_w)

                @pl.when(t >= ring_r)
                def _():
                    pl.semaphore_wait(z_free, 1)

                z_copy(t).start()

            @pl.when(i >= 1)
            def _():
                finish(g * n_ot + 2 * i - 2)
                finish(g * n_ot + 2 * i - 1)

            @pl.when((g == 0) & (lax.rem(i, 3) == 0) & (under(n_hp - 1) + i // 3 < nk))
            def _():
                across_y(nk + under(n_hp - 1) + i // 3)

            return 0

        lax.fori_loop(0, n_ot // 2, project, 0)
        finish(g * n_ot + n_ot - 2)
        finish(g * n_ot + n_ot - 1)
        return 0

    lax.fori_loop(0, 2, group_pass, 0)

    meta_copy.wait_send()
    for o in range(1, n_ep):
        table_copy(o, me).wait_send()
    for u in range(n_unit - 2, n_unit):
        a_copy(u).wait_send()
    for u in range(n_unit - ring_b, n_unit):
        b_copy(u).wait_send()
    for u in range(n_unit - ring_c, n_unit):
        c_copy(u).wait_send()
    for t in range(2 * n_ot - ring_z, 2 * n_ot):
        z_copy(t).wait_send()
        out_copy(t).wait()


def stage(out_local, table, meta, resid, norm_w, w_q, w_k, w_v, w_o, seq_len, n_ep, n_stages, dk=512, bn=256):
    n_exp, capacity, dim = out_local.shape
    n_tok = resid.shape[0]
    cap_dev = capacity // n_ep
    n_slot = n_exp * cap_dev
    width = w_q.shape[1] // 2
    rows_g = n_tok // 2
    n_unit = 2 * dim // dk
    n_w, ring_a, ring_b, ring_c, ring_z, ring_r = 6, 4, 16, 4, 4, 8
    any_spec = pl.BlockSpec(memory_space=pl.ANY)
    vmem_spec = pl.BlockSpec(memory_space=pltpu.VMEM)
    vmem, dma = pltpu.VMEM, pltpu.SemaphoreType.DMA
    return pl.pallas_call(
        functools.partial(stage_kernel, n_ep, n_stages, dk, bn, seq_len),
        out_shape=jax.ShapeDtypeStruct((n_tok, dim), BF16),
        in_specs=[any_spec, vmem_spec, vmem_spec, any_spec, vmem_spec] + [any_spec] * 4,
        out_specs=any_spec,
        scratch_shapes=[
            vmem((n_ep,) + table.shape, F32),
            vmem(meta.shape, F32),
            vmem((n_ep, n_exp, cap_dev, dk), BF16),
            vmem((n_tok, dk), BF16),
            vmem((n_ep, 3 * rows_g, n_slot), BF16),
            vmem((rows_g, n_tok), BF16),
            vmem((2, 2, rows_g, dk), F32),
            vmem((ring_a, 2, rows_g, dk), F32),
            vmem((ring_b, rows_g, dk), F32),
            vmem((ring_b, rows_g, dk), F32),
            vmem((ring_b, rows_g, dk), F32),
            vmem((ring_c, rows_g, dk), BF16),
            vmem((2, rows_g, dim), BF16),
            vmem((2, n_tok, dim), BF16),
            vmem((n_w, dim, bn), BF16),
            vmem((n_tok, width), BF16),
            vmem((n_tok, bn), BF16), vmem((n_tok, bn), BF16), vmem((n_tok, bn), BF16),
            vmem((ring_z, n_tok, bn), F32),
            vmem((ring_r, rows_g, bn), F32),
            vmem((ring_z, rows_g, bn), BF16),
            dma((n_ep,)), dma((1,)), dma((2,)), dma((ring_a,)), dma((ring_b,)), dma((ring_b,)), dma((ring_c,)), dma((n_unit,)),
            dma((rows_g // 32,)), dma((2 * rows_g // 32,)), dma((n_w,)), dma((ring_z,)), dma((ring_r,)), dma((ring_z,)),
            dma((n_ep,)), dma((n_ep,)), dma((1,)), dma((1,)),
            pltpu.SemaphoreType.REGULAR, pltpu.SemaphoreType.REGULAR, pltpu.SemaphoreType.REGULAR,
        ],
        compiler_params=pltpu.CompilerParams(collective_id=0, has_side_effects=True, vmem_limit_bytes=VMEM_LIMIT),
        name='stage',
    )(out_local, table, meta, resid, norm_w, w_q, w_k, w_v, w_o)


def head_tiles(n_tok, width, blk):
    return [(slice(t * blk, (t + 1) * blk), slice(h * HEAD_DIM, (h + 1) * HEAD_DIM)) for h in range(width // HEAD_DIM) for t in range(n_tok // blk)]


def head_scores(q, k, blk=128):
    return [lax.dot_general(q[at], k[at], (((1,), (1,)), ((), ())), preferred_element_type=F32) for at in head_tiles(*q.shape, blk)]


def head_probs(scores, seq_len):
    blk = scores[0].shape[0]
    row = lax.broadcasted_iota(jnp.int32, (blk, blk), 0)
    col = lax.broadcasted_iota(jnp.int32, (blk, blk), 1)
    seen = (row >= col) & (row // seq_len == col // seq_len)
    probs = []
    for s in scores:
        s = jnp.where(seen, s * (HEAD_DIM ** -0.5), -1e30)
        e = jnp.exp(s - jnp.max(s, axis=1, keepdims=True))
        probs.append((e / jnp.sum(e, axis=1, keepdims=True)).astype(BF16))
    return probs


def head_mix(probs, v):
    n_tok, width = v.shape
    blk = probs[0].shape[0]
    tiles = [jnp.dot(p, v[at], preferred_element_type=F32).astype(BF16) for p, at in zip(probs, head_tiles(n_tok, width, blk))]
    per_head = n_tok // blk
    return jnp.concatenate([jnp.concatenate(tiles[h * per_head:(h + 1) * per_head], axis=0) for h in range(width // HEAD_DIM)], axis=1)


def place_kernel(seq_len, src_ref, z_hbm, out_hbm, buf, in_sem, out_sem):
    n_seq = buf.shape[0]

    def take(b):
        return pltpu.make_async_copy(z_hbm.at[pl.ds(pl.multiple_of(src_ref[b] * seq_len, seq_len), seq_len)], buf.at[b], in_sem.at[b])

    def put(b):
        return pltpu.make_async_copy(buf.at[b], out_hbm.at[pl.ds(b * seq_len, seq_len)], out_sem.at[b])

    for b in range(n_seq):
        take(b).start()
    for b in range(n_seq):
        take(b).wait()
        put(b).start()
    for b in range(n_seq):
        put(b).wait()


def place_sequences(src, z, seq_len):
    n_tok, dim = z.shape
    n_seq = n_tok // seq_len
    return pl.pallas_call(
        functools.partial(place_kernel, seq_len),
        in_specs=[pl.BlockSpec(memory_space=pltpu.SMEM), pl.BlockSpec(memory_space=pl.ANY)],
        out_specs=pl.BlockSpec(memory_space=pl.ANY),
        out_shape=jax.ShapeDtypeStruct((n_tok, dim), BF16),
        scratch_shapes=[pltpu.VMEM((n_seq, seq_len, dim), BF16), pltpu.SemaphoreType.DMA((n_seq,)), pltpu.SemaphoreType.DMA((n_seq,))],
        name='place_sequences',
    )(src, z)


def solution(mesh):
    n_stages = mesh.shape['pp']
    n_ep = mesh.shape['ep']
    assert n_stages == 2 and n_ep == 4
    group_axes = ('data', 'pp')

    def device_step(expert_out, expert_id, slot_id, gate, resid, owner, norm_w, w_q, w_k, w_v, w_o):
        me = lax.axis_index('ep')
        out_local, h = expert_out[0, 0], resid[0, 0]
        cap_dev = out_local.shape[1] // n_ep
        n_tok = h.shape[0]
        n_seq = owner.shape[1]
        seq_dev = n_seq // n_ep
        seq_len = n_tok // seq_dev

        ids, slots = expert_id[0, 0].T, slot_id[0, 0].T
        index = jnp.where(slots >= 0, ids * cap_dev + slots - me * cap_dev, -1).astype(F32)
        table = jnp.concatenate([index, gate[0, 0].T], axis=0)

        owned = owner[0].reshape(n_ep, seq_dev)
        sender = owned // seq_dev
        rows = jnp.arange(seq_dev)
        second = jnp.sum((sender[:, :, None] == sender[:, None, :]) & (rows[None, :] < rows[:, None]), axis=2)
        code = (2 * jnp.arange(n_ep)[:, None] + second).reshape(n_seq)
        meta = jnp.sum(jnp.where(owner[0][None, :] == jnp.arange(n_seq)[:, None], code[None, :], 0), axis=1).astype(F32)
        meta = jnp.pad(meta.reshape(n_ep, seq_dev), ((0, 8 - n_ep), (0, 128 - seq_dev)), constant_values=-1)

        z = stage(out_local, table, meta, h, norm_w, w_q[0], w_k[0], w_v[0], w_o[0], seq_len, n_ep, n_stages)

        src = lax.dynamic_index_in_dim(second * n_ep + sender, me, 0, keepdims=False).astype(jnp.int32)
        return place_sequences(src, z, seq_len)[None, None]

    tok_spec = P(group_axes, None, 'ep', None)
    weight_spec = P('pp', None, None)
    in_specs = (P(group_axes, None, 'ep', None, None), tok_spec, tok_spec, tok_spec, tok_spec, P(group_axes, None), P('pp', None), weight_spec,
                weight_spec, weight_spec, weight_spec)
    return jax.shard_map(device_step, mesh=mesh, in_specs=in_specs, out_specs=tok_spec, check_vma=False)
```

```python
import functools

import jax
import jax.numpy as jnp
from jax import lax
from jax.experimental import pallas as pl
from jax.experimental.pallas import tpu as pltpu
from jax.sharding import PartitionSpec as P

HEAD_DIM = 128
NORM_EPS = 1e-6
F32, BF16 = jnp.float32, jnp.bfloat16
MESH = pl.DeviceIdType.MESH
VMEM_LIMIT = 67_043_328


def stage_kernel(n_ep, n_stages, dk, bn, seq_len, o_hbm, ids_ref, slots_ref, gate_ref, own_ref, h_hbm, nw_ref, wq_hbm, wk_hbm, wv_hbm, wo_hbm, z_hbm, table_mine, meta_mine, tables, meta, obuf, hbuf, w3, perm,
                 send_a, recv_a, keep, send_b, recv_b, send_c, y_own, xbuf, wbuf, abuf, q_scr, k_scr, v_scr, zscr, recv_z, zout,
                 o_sem, h_sem, sa_sem, ra_sem, sb_sem, rb_sem, sc_sem, rc_sem, sx_sem, rx_sem, w_sem, sz_sem, rz_sem, out_sem,
                 st_sem, rt_sem, sm_sem, rm_sem, a_free, b_free, z_free):
    me = lax.axis_index('ep')
    rank = lax.axis_index('pp')
    core = lax.rem(me, 2)
    core_peer = me + 1 - 2 * core
    x_peer = lax.rem(me + 2, n_ep)
    other_rank = 1 - rank
    n_exp, cap_dev, n_slot = obuf.shape[1], obuf.shape[2], perm.shape[1] * 3
    n_tok, dim = h_hbm.shape
    n_slot = n_exp * cap_dev
    rows_g = n_tok // 2
    sub = rows_g // n_ep
    nk = dim // dk
    n_unit = 2 * nk
    ring_a, ring_b, ring_c = recv_a.shape[0], keep.shape[0], send_c.shape[0]
    width = abuf.shape[1]
    n_hp = width // bn
    n_ot = dim // bn
    n_w, ring_z, ring_r = wbuf.shape[0], zscr.shape[0], recv_z.shape[0]
    n_tile = 3 * n_hp + n_ot

    def col(k, w):
        return pl.ds(pl.multiple_of(k * w, w), w)

    def o_copy(u, o):
        j = lax.rem(me + o, n_ep)
        return pltpu.make_async_copy(o_hbm.at[:, col(j, cap_dev), col(lax.rem(u, nk), dk)], obuf.at[o], o_sem.at[o])

    def h_copy(u):
        return pltpu.make_async_copy(h_hbm.at[:, col(lax.rem(u, nk), dk)], hbuf, h_sem.at[0])

    def to_core(src, dst, s_sem, r_sem):
        return pltpu.make_async_remote_copy(src, dst, s_sem, r_sem, device_id={'ep': core_peer}, device_id_type=MESH)

    def a_copy(u):
        return to_core(send_a.at[lax.rem(u, 2)], recv_a.at[lax.rem(u, ring_a)], sa_sem.at[lax.rem(u, 2)], ra_sem.at[lax.rem(u, ring_a)])

    def b_copy(u):
        i = lax.rem(u, ring_b)
        return pltpu.make_async_remote_copy(send_b.at[i], recv_b.at[i], sb_sem.at[i], rb_sem.at[i], device_id={'ep': x_peer}, device_id_type=MESH)

    def c_copy(u):
        i = lax.rem(u, ring_c)
        return pltpu.make_async_remote_copy(send_c.at[i], y_own.at[u // nk, :, col(lax.rem(u, nk), dk)], sc_sem.at[i], rc_sem.at[u],
                                            device_id={'pp': other_rank}, device_id_type=MESH)

    def x_copy(g, p):
        at = xbuf.at[g, pl.ds(pl.multiple_of(core * rows_g + p * 32, 32), 32)]
        return to_core(at, at, sx_sem.at[p], rx_sem.at[g * (rows_g // 32) + p])

    def z_copy(t):
        theirs = pl.ds(pl.multiple_of((1 - core) * rows_g, rows_g), rows_g)
        return to_core(zscr.at[lax.rem(t, ring_z), theirs], recv_z.at[lax.rem(t, ring_r)], sz_sem.at[lax.rem(t, ring_z)], rz_sem.at[lax.rem(t, ring_r)])

    def out_copy(t):
        i = lax.rem(t, ring_z)
        return pltpu.make_async_copy(zout.at[i], z_hbm.at[col(t // n_ot, rows_g), col(lax.rem(t, n_ot), bn)], out_sem.at[i])

    def w_slot(s):
        return wbuf.at[lax.rem(s, n_w)], w_sem.at[lax.rem(s, n_w)]

    def qkv_tile(s, hp, kind):
        slot, sem = w_slot(s)
        return pltpu.make_async_copy((wq_hbm, wk_hbm, wv_hbm)[kind].at[:, col(core * n_hp + hp, bn)], slot, sem)

    def out_tile(s, t):
        slot, sem = w_slot(s)
        return pltpu.make_async_copy(wo_hbm.at[col(core, width), col(t, bn)], slot.at[pl.ds(0, width)], sem)

    def start_tile(s):
        at = lax.rem(s, n_tile)

        @pl.when(s < 2 * n_tile)
        def _():
            for kind in range(3):
                @pl.when((at < 3 * n_hp) & (lax.rem(at, 3) == kind))
                def _():
                    qkv_tile(s, at // 3, kind).start()

            @pl.when(at >= 3 * n_hp)
            def _():
                out_tile(s, at - 3 * n_hp).start()

    for o in range(n_ep):
        o_copy(0, o).start()
    h_copy(0).start()
    barrier = pltpu.get_barrier_semaphore()
    for o in range(1, n_ep):
        pl.semaphore_signal(barrier, inc=1, device_id={'ep': lax.rem(me + o, n_ep)}, device_id_type=MESH)
    pl.semaphore_signal(barrier, inc=1, device_id={'pp': other_rank}, device_id_type=MESH)

    def table_copy(o, source):
        return pltpu.make_async_remote_copy(table_mine, tables.at[source], st_sem.at[o], rt_sem.at[source],
                                            device_id={'ep': lax.rem(me + o, n_ep)}, device_id_type=MESH)

    meta_copy = pltpu.make_async_remote_copy(meta_mine, meta, sm_sem.at[0], rm_sem.at[0], device_id={'pp': other_rank}, device_id_type=MESH)

    def tabulate():
        slots = slots_ref[...]
        table_mine[0:8, :] = jnp.where(slots >= 0, ids_ref[...] * cap_dev + slots - me * cap_dev, -1).astype(F32)
        table_mine[8:16, :] = gate_ref[...]
        n_seq = own_ref.shape[1]
        seq_dev = n_seq // n_ep
        down = lax.broadcasted_iota(jnp.int32, (n_seq, n_seq), 0)
        across = lax.broadcasted_iota(jnp.int32, (n_seq, n_seq), 1)

        def part(x):
            return sum((x >= seq_dev * d).astype(F32) for d in range(1, n_ep))

        own = jnp.broadcast_to(own_ref[...], (n_seq, n_seq)).astype(F32)
        own_down = jnp.sum(jnp.where(down == across, own, 0.0), axis=1, keepdims=True)
        earlier = (part(own_down) == part(own)) & (down < across) & (part(down) == part(across))
        second = jnp.sum(earlier.astype(F32), axis=0, keepdims=True)
        code = 2 * part(across) + second
        code = jnp.sum(jnp.where(own == down.astype(F32), code, 0.0), axis=1, keepdims=True)
        meta_mine[...] = jnp.broadcast_to(code, meta_mine.shape)

    def build(g, o):
        j = lax.rem(me + o, n_ep)
        slot = lax.broadcasted_iota(jnp.int32, (sub, n_slot), 1).astype(F32) + (me * n_slot).astype(F32)
        table = tables[j].T
        wide = (sub, table.shape[1])
        n_q = n_tok // sub
        block = meta[pl.ds(pl.multiple_of(j * n_q, n_q), n_q), :]
        codes = [jnp.broadcast_to(block[q:q + 1, :wide[1]], wide) for q in range(n_q)]
        x_me = me // 2
        for r in range(n_ep):
            dest = 2 * (x_me if r % 2 == 0 else 1 - x_me) + (core if r < 2 else 1 - core)
            want = (2 * dest + g).astype(F32)
            rows = jnp.zeros(wide, F32)
            for q in range(n_q):
                rows = jnp.where(codes[q] == want, table[q * sub:(q + 1) * sub], rows)
            w = jnp.zeros((sub, n_slot), F32)
            for c in range(8):
                w = jnp.where(rows[:, c:c + 1] == slot, rows[:, 8 + c:9 + c], w)
            for t in range(3):
                high = w.astype(BF16)
                w3[o, t * rows_g + r * sub:t * rows_g + (r + 1) * sub, :] = high
                w = w - high.astype(F32)
            if o == 0:
                home = jnp.zeros(wide, F32)
                for q in range(n_q):
                    home = jnp.where(codes[q] == want, float(q * sub), home)
                token = lax.broadcasted_iota(jnp.int32, (sub, n_tok), 1)
                line = lax.broadcasted_iota(jnp.int32, (sub, n_tok), 0)
                perm[r * sub:(r + 1) * sub, :] = (home[:, 0:1] == (token - line).astype(F32)).astype(F32).astype(BF16)

    def partial_sums(u):
        @pl.when(u >= 2)
        def _():
            a_copy(u - 2).wait_send()

        @pl.when(u >= ring_b)
        def _():
            b_copy(u - ring_b).wait_send()

        for o in range(n_ep):
            @pl.when(lax.rem(u, nk) == 0)
            def _():
                @pl.when(u == 0)
                def _():
                    if o == 0:
                        meta_copy.wait_recv()
                    else:
                        table_copy(o, lax.rem(me + o, n_ep)).wait_recv()

                build(u // nk, o)

            o_copy(u, o).wait()
            rows = obuf[o].reshape(n_slot, dk)
            split = jnp.dot(w3[o], rows, preferred_element_type=F32)
            part = split[:rows_g] + split[rows_g:2 * rows_g] + split[2 * rows_g:]
            if o == 0:
                h_copy(u).wait()
                part += jnp.dot(perm[...], hbuf[...], preferred_element_type=F32)
            place = pl.ds(pl.multiple_of(lax.rem(me + o, n_ep) * sub, sub), sub)
            keep[lax.rem(u, ring_b), place, :] = part[0:sub]
            send_b[lax.rem(u, ring_b), place, :] = part[sub:2 * sub]
            send_a[lax.rem(u, 2), 0, place, :] = part[2 * sub:3 * sub]
            send_a[lax.rem(u, 2), 1, place, :] = part[3 * sub:4 * sub]

            @pl.when(u + 1 < n_unit)
            def _():
                o_copy(u + 1, o).start()
                if o == 0:
                    h_copy(u + 1).start()

        @pl.when(u >= ring_a)
        def _():
            pl.semaphore_wait(a_free, 1)

        a_copy(u).start()

    def across_x(u):
        i = lax.rem(u, ring_b)
        a_copy(u).wait_recv()
        keep[i] = keep[i] + recv_a[lax.rem(u, ring_a), 0]
        send_b[i] = send_b[i] + recv_a[lax.rem(u, ring_a), 1]

        @pl.when(u < n_unit - ring_a)
        def _():
            pl.semaphore_signal(a_free, inc=1, device_id={'ep': core_peer}, device_id_type=MESH)

        @pl.when(u >= ring_b)
        def _():
            pl.semaphore_wait(b_free, 1)

        b_copy(u).start()

    def across_y(u):
        i = lax.rem(u, ring_b)
        b_copy(u).wait_recv()

        @pl.when(u >= ring_c)
        def _():
            c_copy(u - ring_c).wait_send()

        send_c[lax.rem(u, ring_c)] = (keep[i] + recv_b[i]).astype(BF16)
        c_copy(u).start()

        @pl.when(u < n_unit - ring_b)
        def _():
            pl.semaphore_signal(b_free, inc=1, device_id={'ep': x_peer}, device_id_type=MESH)

    tabulate()
    pl.semaphore_wait(barrier, n_ep)
    meta_copy.start()
    for o in range(1, n_ep):
        table_copy(o, me).start()
    tables[me] = table_mine[...]
    ahead = nk

    def phase_one(u, _):
        @pl.when(u < n_unit)
        def _():
            partial_sums(u)

        @pl.when((u >= 2) & (u < 2 + n_w))
        def _():
            start_tile(u - 2)

        @pl.when(u >= 1)
        def _():
            across_x(u - 1)

        @pl.when((u >= 2) & (lax.rem(u, 2) == 0))
        def _():
            across_y(u // 2 - 1)

        return 0

    lax.fori_loop(0, n_unit + 1, phase_one, 0)

    def attend(hp):
        abuf[:, col(hp, bn)] = head_mix(head_probs(head_scores(q_scr[...], k_scr[...]), seq_len), v_scr[...])

    q_scr[...] = jnp.zeros_like(q_scr)
    k_scr[...] = jnp.zeros_like(k_scr)
    v_scr[...] = jnp.zeros_like(v_scr)

    def under(hp):
        return (hp + 1) * 3 // 5 if isinstance(hp, int) else lax.div((hp + 1) * 3, 5)

    n_last = max(0, nk - under(n_hp - 1) - (n_ot // 2 + 2) // 3)

    def finish(t):
        g, i = t // n_ot, lax.rem(t, ring_z)
        mine = pl.ds(pl.multiple_of(core * rows_g, rows_g), rows_g)
        z_copy(t).wait_recv()
        proj = (zscr[i, mine, :] + recv_z[lax.rem(t, ring_r)]).astype(BF16)

        @pl.when(t < 2 * n_ot - ring_r)
        def _():
            pl.semaphore_signal(z_free, inc=1, device_id={'ep': core_peer}, device_id_type=MESH)

        @pl.when(t >= ring_z)
        def _():
            out_copy(t - ring_z).wait()

        zout[i] = (y_own[g, :, col(lax.rem(t, n_ot), bn)].astype(F32) + proj.astype(F32)).astype(BF16)
        out_copy(t).start()

    def group_pass(g, _):
        def late(u, _):
            across_y(u)
            return 0

        lax.fori_loop(jnp.where(g == 0, ahead, n_unit - n_last), jnp.where(g == 0, nk, n_unit), late, 0)

        def arrived(k, _):
            c_copy(g * nk + k).wait_recv()
            return 0

        lax.fori_loop(0, nk, arrived, 0)

        def norm(p, _):
            for half in range(2):
                y = y_own[g, pl.ds(pl.multiple_of(p * 32 + half * 16, 16), 16), :].astype(F32)
                inv = lax.rsqrt(jnp.mean(y * y, axis=1, keepdims=True) + NORM_EPS)
                xbuf[g, pl.ds(pl.multiple_of(core * rows_g + p * 32 + half * 16, 16), 16), :] = (y * inv * nw_ref[...]).astype(BF16)
            x_copy(g, p).start()
            return 0

        lax.fori_loop(0, rows_g // 32, norm, 0)

        def exchanged(p, _):
            x_copy(g, p).wait()
            return 0

        lax.fori_loop(0, rows_g // 32, exchanged, 0)

        def heads(hp, _):
            s = g * n_tile + hp * 3
            for kind in range(3):
                qkv_tile(s + kind, hp, kind).wait()
            scores = head_scores(q_scr[...], k_scr[...])
            q = jnp.dot(xbuf[g], wbuf[lax.rem(s, n_w)], preferred_element_type=F32).astype(BF16)
            mixed = head_mix(head_probs(scores, seq_len), v_scr[...])
            k = jnp.dot(xbuf[g], wbuf[lax.rem(s + 1, n_w)], preferred_element_type=F32).astype(BF16)
            v = jnp.dot(xbuf[g], wbuf[lax.rem(s + 2, n_w)], preferred_element_type=F32).astype(BF16)
            abuf[:, col(jnp.maximum(hp - 1, 0), bn)] = mixed
            q_scr[...] = q
            k_scr[...] = k
            v_scr[...] = v
            for kind in range(3):
                start_tile(s + kind + n_w)

            @pl.when((g == 0) & (under(hp) > under(hp - 1)))
            def _():
                across_y(nk + under(hp) - 1)

            return 0

        lax.fori_loop(0, n_hp, heads, 0)
        attend(n_hp - 1)

        def project(i, _):
            for r in range(2):
                t = g * n_ot + 2 * i + r
                s = g * n_tile + 3 * n_hp + 2 * i + r

                @pl.when(t >= ring_z)
                def _():
                    z_copy(t - ring_z).wait_send()

                out_tile(s, 2 * i + r).wait()
            for r in range(2):
                t = g * n_ot + 2 * i + r
                s = g * n_tile + 3 * n_hp + 2 * i + r
                zscr[lax.rem(t, ring_z)] = jnp.dot(abuf[...], wbuf[lax.rem(s, n_w), 0:width, :], preferred_element_type=F32)
            for r in range(2):
                t = g * n_ot + 2 * i + r
                start_tile(g * n_tile + 3 * n_hp + 2 * i + r + n_w)

                @pl.when(t >= ring_r)
                def _():
                    pl.semaphore_wait(z_free, 1)

                z_copy(t).start()

            @pl.when(i >= 1)
            def _():
                finish(g * n_ot + 2 * i - 2)
                finish(g * n_ot + 2 * i - 1)

            @pl.when((g == 0) & (lax.rem(i, 3) == 0) & (under(n_hp - 1) + i // 3 < nk))
            def _():
                across_y(nk + under(n_hp - 1) + i // 3)

            return 0

        lax.fori_loop(0, n_ot // 2, project, 0)
        finish(g * n_ot + n_ot - 2)
        finish(g * n_ot + n_ot - 1)
        return 0

    lax.fori_loop(0, 2, group_pass, 0)

    meta_copy.wait_send()
    for o in range(1, n_ep):
        table_copy(o, me).wait_send()
    for u in range(n_unit - 2, n_unit):
        a_copy(u).wait_send()
    for u in range(n_unit - ring_b, n_unit):
        b_copy(u).wait_send()
    for u in range(n_unit - ring_c, n_unit):
        c_copy(u).wait_send()
    for t in range(2 * n_ot - ring_z, 2 * n_ot):
        z_copy(t).wait_send()
        out_copy(t).wait()


def stage(out_local, ids, slots, gate, owner, resid, norm_w, w_q, w_k, w_v, w_o, seq_len, n_ep, n_stages, dk=512, bn=256):
    n_exp, capacity, dim = out_local.shape
    n_tok = resid.shape[0]
    cap_dev = capacity // n_ep
    n_slot = n_exp * cap_dev
    width = w_q.shape[1] // 2
    rows_g = n_tok // 2
    n_unit = 2 * dim // dk
    n_w, ring_a, ring_b, ring_c, ring_z, ring_r = 7, 3, 15, 2, 4, 4
    any_spec = pl.BlockSpec(memory_space=pl.ANY)
    vmem_spec = pl.BlockSpec(memory_space=pltpu.VMEM)
    vmem, dma = pltpu.VMEM, pltpu.SemaphoreType.DMA
    return pl.pallas_call(
        functools.partial(stage_kernel, n_ep, n_stages, dk, bn, seq_len),
        out_shape=jax.ShapeDtypeStruct((n_tok, dim), BF16),
        in_specs=[any_spec, vmem_spec, vmem_spec, vmem_spec, vmem_spec, any_spec, vmem_spec] + [any_spec] * 4,
        out_specs=any_spec,
        scratch_shapes=[
            vmem((2 * ids.shape[0], n_tok), F32),
            vmem((owner.shape[1], 128), F32),
            vmem((n_ep, 2 * ids.shape[0], n_tok), F32),
            vmem((owner.shape[1], 128), F32),
            vmem((n_ep, n_exp, cap_dev, dk), BF16),
            vmem((n_tok, dk), BF16),
            vmem((n_ep, 3 * rows_g, n_slot), BF16),
            vmem((rows_g, n_tok), BF16),
            vmem((2, 2, rows_g, dk), F32),
            vmem((ring_a, 2, rows_g, dk), F32),
            vmem((ring_b, rows_g, dk), F32),
            vmem((ring_b, rows_g, dk), F32),
            vmem((ring_b, rows_g, dk), F32),
            vmem((ring_c, rows_g, dk), BF16),
            vmem((2, rows_g, dim), BF16),
            vmem((2, n_tok, dim), BF16),
            vmem((n_w, dim, bn), BF16),
            vmem((n_tok, width), BF16),
            vmem((n_tok, bn), BF16), vmem((n_tok, bn), BF16), vmem((n_tok, bn), BF16),
            vmem((ring_z, n_tok, bn), F32),
            vmem((ring_r, rows_g, bn), F32),
            vmem((ring_z, rows_g, bn), BF16),
            dma((n_ep,)), dma((1,)), dma((2,)), dma((ring_a,)), dma((ring_b,)), dma((ring_b,)), dma((ring_c,)), dma((n_unit,)),
            dma((rows_g // 32,)), dma((2 * rows_g // 32,)), dma((n_w,)), dma((ring_z,)), dma((ring_r,)), dma((ring_z,)),
            dma((n_ep,)), dma((n_ep,)), dma((1,)), dma((1,)),
            pltpu.SemaphoreType.REGULAR, pltpu.SemaphoreType.REGULAR, pltpu.SemaphoreType.REGULAR,
        ],
        compiler_params=pltpu.CompilerParams(collective_id=0, has_side_effects=True, vmem_limit_bytes=VMEM_LIMIT),
        name='stage',
    )(out_local, ids, slots, gate, owner, resid, norm_w, w_q, w_k, w_v, w_o)


def head_tiles(n_tok, width, blk):
    return [(slice(t * blk, (t + 1) * blk), slice(h * HEAD_DIM, (h + 1) * HEAD_DIM)) for h in range(width // HEAD_DIM) for t in range(n_tok // blk)]


def head_scores(q, k, blk=128):
    return [lax.dot_general(q[at], k[at], (((1,), (1,)), ((), ())), preferred_element_type=F32) for at in head_tiles(*q.shape, blk)]


def head_probs(scores, seq_len):
    blk = scores[0].shape[0]
    row = lax.broadcasted_iota(jnp.int32, (blk, blk), 0)
    col = lax.broadcasted_iota(jnp.int32, (blk, blk), 1)
    seen = (row >= col) & (row // seq_len == col // seq_len)
    probs = []
    for s in scores:
        s = jnp.where(seen, s * (HEAD_DIM ** -0.5), -1e30)
        e = jnp.exp(s - jnp.max(s, axis=1, keepdims=True))
        probs.append((e / jnp.sum(e, axis=1, keepdims=True)).astype(BF16))
    return probs


def head_mix(probs, v):
    n_tok, width = v.shape
    blk = probs[0].shape[0]
    tiles = [jnp.dot(p, v[at], preferred_element_type=F32).astype(BF16) for p, at in zip(probs, head_tiles(n_tok, width, blk))]
    per_head = n_tok // blk
    return jnp.concatenate([jnp.concatenate(tiles[h * per_head:(h + 1) * per_head], axis=0) for h in range(width // HEAD_DIM)], axis=1)


def place_kernel(seq_len, n_ep, own_ref, z_hbm, out_hbm, buf, in_sem, out_sem):
    n_seq = buf.shape[0]
    me = lax.axis_index('ep')
    sender = [own_ref[0, me * n_seq + b] // n_seq for b in range(n_seq)]

    def take(b):
        second = sum([(sender[a] == sender[b]).astype(jnp.int32) for a in range(b)], jnp.int32(0))
        row = pl.multiple_of((second * n_ep + sender[b]) * seq_len, seq_len)
        return pltpu.make_async_copy(z_hbm.at[pl.ds(row, seq_len)], buf.at[b], in_sem.at[b])

    def put(b):
        return pltpu.make_async_copy(buf.at[b], out_hbm.at[pl.ds(b * seq_len, seq_len)], out_sem.at[b])

    for b in range(n_seq):
        take(b).start()
    for b in range(n_seq):
        take(b).wait()
        put(b).start()
    for b in range(n_seq):
        put(b).wait()


def place_sequences(owner, z, seq_len, n_ep):
    n_tok, dim = z.shape
    n_seq = n_tok // seq_len
    return pl.pallas_call(
        functools.partial(place_kernel, seq_len, n_ep),
        in_specs=[pl.BlockSpec(memory_space=pltpu.SMEM), pl.BlockSpec(memory_space=pl.ANY)],
        out_specs=pl.BlockSpec(memory_space=pl.ANY),
        out_shape=jax.ShapeDtypeStruct((n_tok, dim), BF16),
        scratch_shapes=[pltpu.VMEM((n_seq, seq_len, dim), BF16), pltpu.SemaphoreType.DMA((n_seq,)), pltpu.SemaphoreType.DMA((n_seq,))],
        name='place_sequences',
    )(owner, z)


def solution(mesh):
    n_stages = mesh.shape['pp']
    n_ep = mesh.shape['ep']
    assert n_stages == 2 and n_ep == 4
    group_axes = ('data', 'pp')

    def device_step(expert_out, expert_id, slot_id, gate, resid, owner, norm_w, w_q, w_k, w_v, w_o):
        n_tok = resid.shape[2]
        seq_len = n_tok * n_ep // owner.shape[1]
        z = stage(expert_out[0, 0], expert_id[0, 0].T, slot_id[0, 0].T, gate[0, 0].T, owner, resid[0, 0], norm_w, w_q[0], w_k[0], w_v[0], w_o[0],
                  seq_len, n_ep, n_stages)
        return place_sequences(owner, z, seq_len, n_ep)[None, None]

    tok_spec = P(group_axes, None, 'ep', None)
    weight_spec = P('pp', None, None)
    in_specs = (P(group_axes, None, 'ep', None, None), tok_spec, tok_spec, tok_spec, tok_spec, P(group_axes, None), P('pp', None), weight_spec,
                weight_spec, weight_spec, weight_spec)
    return jax.shard_map(device_step, mesh=mesh, in_specs=in_specs, out_specs=tok_spec, check_vma=False)
```

```python
import functools

import jax
import jax.numpy as jnp
from jax import lax
from jax.experimental import pallas as pl
from jax.experimental.pallas import tpu as pltpu
from jax.sharding import PartitionSpec as P

HEAD_DIM = 128
NORM_EPS = 1e-6
F32, BF16 = jnp.float32, jnp.bfloat16
MESH = pl.DeviceIdType.MESH
VMEM_LIMIT = 67_043_328


def stage_kernel(n_ep, n_stages, dk, bn, seq_len, o_hbm, ids_ref, slots_ref, gate_ref, own_ref, h_hbm, nw_ref, wq_hbm, wk_hbm, wv_hbm, wo_hbm, z_hbm, table_mine, meta_mine, tables, meta, obuf, hbuf, w3, perm,
                 send_a, recv_a, keep, send_b, recv_b, send_c, y_own, xbuf, wbuf, abuf, q_scr, k_scr, v_scr, zscr, recv_z, zout,
                 o_sem, h_sem, sa_sem, ra_sem, sb_sem, rb_sem, sc_sem, rc_sem, sx_sem, rx_sem, w_sem, sz_sem, rz_sem, out_sem,
                 st_sem, rt_sem, sm_sem, rm_sem, a_free, b_free, z_free):
    me = lax.axis_index('ep')
    rank = lax.axis_index('pp')
    core = lax.rem(me, 2)
    core_peer = me + 1 - 2 * core
    x_peer = lax.rem(me + 2, n_ep)
    other_rank = 1 - rank
    n_exp, cap_dev, n_slot = obuf.shape[1], obuf.shape[2], perm.shape[1] * 3
    n_tok, dim = h_hbm.shape
    n_slot = n_exp * cap_dev
    rows_g = n_tok // 2
    sub = rows_g // n_ep
    nk = dim // dk
    n_unit = 2 * nk
    ring_a, ring_b, ring_c = recv_a.shape[0], keep.shape[0], send_c.shape[0]
    width = abuf.shape[1]
    n_hp = width // bn
    n_ot = dim // bn
    n_w, ring_z, ring_r, ring_o = wbuf.shape[0], zscr.shape[0], recv_z.shape[0], zout.shape[0]
    n_tile = 3 * n_hp + n_ot

    def col(k, w):
        return pl.ds(pl.multiple_of(k * w, w), w)

    def o_copy(u, o):
        j = lax.rem(me + o, n_ep)
        return pltpu.make_async_copy(o_hbm.at[:, col(j, cap_dev), col(lax.rem(u, nk), dk)], obuf.at[o], o_sem.at[o])

    def h_copy(u):
        return pltpu.make_async_copy(h_hbm.at[:, col(lax.rem(u, nk), dk)], hbuf, h_sem.at[0])

    def to_core(src, dst, s_sem, r_sem):
        return pltpu.make_async_remote_copy(src, dst, s_sem, r_sem, device_id={'ep': core_peer}, device_id_type=MESH)

    def a_copy(u):
        return to_core(send_a.at[lax.rem(u, 2)], recv_a.at[lax.rem(u, ring_a)], sa_sem.at[lax.rem(u, 2)], ra_sem.at[lax.rem(u, ring_a)])

    halves = [slice(0, rows_g // 2), slice(rows_g // 2, rows_g)]

    def b_copy(u, h):
        i = lax.rem(u, ring_b)
        return pltpu.make_async_remote_copy(send_b.at[i, halves[h]], recv_b.at[i, halves[h]], sb_sem.at[2 * i + h], rb_sem.at[2 * i + h],
                                            device_id={'ep': x_peer}, device_id_type=MESH)

    def c_copy(u, h):
        i = lax.rem(u, ring_c)
        return pltpu.make_async_remote_copy(send_c.at[i, halves[h]], y_own.at[u // nk, halves[h], col(lax.rem(u, nk), dk)], sc_sem.at[2 * i + h],
                                            rc_sem.at[2 * u + h], device_id={'pp': other_rank}, device_id_type=MESH)

    def x_copy(g, p):
        at = xbuf.at[g, pl.ds(pl.multiple_of(core * rows_g + p * 32, 32), 32)]
        return to_core(at, at, sx_sem.at[p], rx_sem.at[g * (rows_g // 32) + p])

    def z_copy(t):
        theirs = pl.ds(pl.multiple_of((1 - core) * rows_g, rows_g), rows_g)
        return to_core(zscr.at[lax.rem(t, ring_z), theirs], recv_z.at[lax.rem(t, ring_r)], sz_sem.at[lax.rem(t, ring_z)], rz_sem.at[lax.rem(t, ring_r)])

    def out_copy(t):
        i = lax.rem(t, ring_o)
        return pltpu.make_async_copy(zout.at[i], z_hbm.at[col(t // n_ot, rows_g), col(lax.rem(t, n_ot), bn)], out_sem.at[i])

    def w_slot(s):
        return wbuf.at[lax.rem(s, n_w)], w_sem.at[lax.rem(s, n_w)]

    def qkv_tile(s, hp, kind):
        slot, sem = w_slot(s)
        return pltpu.make_async_copy((wq_hbm, wk_hbm, wv_hbm)[kind].at[:, col(core * n_hp + hp, bn)], slot, sem)

    def out_tile(s, t):
        slot, sem = w_slot(s)
        return pltpu.make_async_copy(wo_hbm.at[col(core, width), col(t, bn)], slot.at[pl.ds(0, width)], sem)

    def start_tile(s):
        at = lax.rem(s, n_tile)

        @pl.when(s < 2 * n_tile)
        def _():
            for kind in range(3):
                @pl.when((at < 3 * n_hp) & (lax.rem(at, 3) == kind))
                def _():
                    qkv_tile(s, at // 3, kind).start()

            @pl.when(at >= 3 * n_hp)
            def _():
                out_tile(s, at - 3 * n_hp).start()

    for o in range(n_ep):
        o_copy(0, o).start()
    h_copy(0).start()
    barrier = pltpu.get_barrier_semaphore()
    for o in range(1, n_ep):
        pl.semaphore_signal(barrier, inc=1, device_id={'ep': lax.rem(me + o, n_ep)}, device_id_type=MESH)
    pl.semaphore_signal(barrier, inc=1, device_id={'pp': other_rank}, device_id_type=MESH)

    def table_copy(o, source):
        return pltpu.make_async_remote_copy(table_mine, tables.at[source], st_sem.at[o], rt_sem.at[source],
                                            device_id={'ep': lax.rem(me + o, n_ep)}, device_id_type=MESH)

    meta_copy = pltpu.make_async_remote_copy(meta_mine, meta, sm_sem.at[0], rm_sem.at[0], device_id={'pp': other_rank}, device_id_type=MESH)

    def tabulate():
        slots = slots_ref[...]
        table_mine[0:8, :] = jnp.where(slots >= 0, ids_ref[...] * cap_dev + slots - me * cap_dev, -1).astype(F32)
        table_mine[8:16, :] = gate_ref[...]
        n_seq = own_ref.shape[1]
        seq_dev = n_seq // n_ep
        down = lax.broadcasted_iota(jnp.int32, (n_seq, n_seq), 0)
        across = lax.broadcasted_iota(jnp.int32, (n_seq, n_seq), 1)

        def part(x):
            return sum((x >= seq_dev * d).astype(F32) for d in range(1, n_ep))

        own = jnp.broadcast_to(own_ref[...], (n_seq, n_seq)).astype(F32)
        own_down = jnp.sum(jnp.where(down == across, own, 0.0), axis=1, keepdims=True)
        earlier = (part(own_down) == part(own)) & (down < across) & (part(down) == part(across))
        second = jnp.sum(earlier.astype(F32), axis=0, keepdims=True)
        code = 2 * part(across) + second
        code = jnp.sum(jnp.where(own == down.astype(F32), code, 0.0), axis=1, keepdims=True)
        meta_mine[...] = jnp.broadcast_to(code, meta_mine.shape)

    def build(g, o):
        j = lax.rem(me + o, n_ep)
        slot = lax.broadcasted_iota(jnp.int32, (sub, n_slot), 1).astype(F32) + (me * n_slot).astype(F32)
        table = tables[j].T
        wide = (sub, table.shape[1])
        n_q = n_tok // sub
        block = meta[pl.ds(pl.multiple_of(j * n_q, n_q), n_q), :]
        codes = [jnp.broadcast_to(block[q:q + 1, :wide[1]], wide) for q in range(n_q)]
        x_me = me // 2
        for r in range(n_ep):
            dest = 2 * (x_me if r % 2 == 0 else 1 - x_me) + (core if r < 2 else 1 - core)
            want = (2 * dest + g).astype(F32)
            rows = jnp.zeros(wide, F32)
            for q in range(n_q):
                rows = jnp.where(codes[q] == want, table[q * sub:(q + 1) * sub], rows)
            w = jnp.zeros((sub, n_slot), F32)
            for c in range(8):
                w = jnp.where(rows[:, c:c + 1] == slot, rows[:, 8 + c:9 + c], w)
            for t in range(3):
                high = w.astype(BF16)
                w3[o, t * rows_g + r * sub:t * rows_g + (r + 1) * sub, :] = high
                w = w - high.astype(F32)
            if o == 0:
                home = jnp.zeros(wide, F32)
                for q in range(n_q):
                    home = jnp.where(codes[q] == want, float(q * sub), home)
                token = lax.broadcasted_iota(jnp.int32, (sub, n_tok), 1)
                line = lax.broadcasted_iota(jnp.int32, (sub, n_tok), 0)
                perm[r * sub:(r + 1) * sub, :] = (home[:, 0:1] == (token - line).astype(F32)).astype(F32).astype(BF16)

    def partial_sums(u):
        @pl.when(u >= 2)
        def _():
            a_copy(u - 2).wait_send()

        @pl.when(u >= ring_b)
        def _():
            for h in range(2):
                b_copy(u - ring_b, h).wait_send()

        for o in range(n_ep):
            @pl.when(lax.rem(u, nk) == 0)
            def _():
                @pl.when(u == 0)
                def _():
                    if o == 0:
                        meta_copy.wait_recv()
                    else:
                        table_copy(o, lax.rem(me + o, n_ep)).wait_recv()

                build(u // nk, o)

            o_copy(u, o).wait()
            rows = obuf[o].reshape(n_slot, dk)
            split = jnp.dot(w3[o], rows, preferred_element_type=F32)
            part = split[:rows_g] + split[rows_g:2 * rows_g] + split[2 * rows_g:]
            if o == 0:
                h_copy(u).wait()
                part += jnp.dot(perm[...], hbuf[...], preferred_element_type=F32)
            place = pl.ds(pl.multiple_of(lax.rem(me + o, n_ep) * sub, sub), sub)
            keep[lax.rem(u, ring_b), place, :] = part[0:sub]
            send_b[lax.rem(u, ring_b), place, :] = part[sub:2 * sub]
            send_a[lax.rem(u, 2), 0, place, :] = part[2 * sub:3 * sub]
            send_a[lax.rem(u, 2), 1, place, :] = part[3 * sub:4 * sub]

            @pl.when(u + 1 < n_unit)
            def _():
                o_copy(u + 1, o).start()
                if o == 0:
                    h_copy(u + 1).start()

        @pl.when(u >= ring_a)
        def _():
            pl.semaphore_wait(a_free, 1)

        a_copy(u).start()

    def across_x(u):
        i = lax.rem(u, ring_b)
        a_copy(u).wait_recv()
        keep[i] = keep[i] + recv_a[lax.rem(u, ring_a), 0]
        send_b[i] = send_b[i] + recv_a[lax.rem(u, ring_a), 1]

        @pl.when(u < n_unit - ring_a)
        def _():
            pl.semaphore_signal(a_free, inc=1, device_id={'ep': core_peer}, device_id_type=MESH)

        @pl.when(u >= ring_b)
        def _():
            pl.semaphore_wait(b_free, 1)

        for h in range(2):
            b_copy(u, h).start()

    def across_y(u):
        i = lax.rem(u, ring_b)
        for h in range(2):
            b_copy(u, h).wait_recv()

            @pl.when(u >= ring_c)
            def _():
                c_copy(u - ring_c, h).wait_send()

            send_c[lax.rem(u, ring_c), halves[h]] = (keep[i, halves[h]] + recv_b[i, halves[h]]).astype(BF16)
            c_copy(u, h).start()

        @pl.when(u < n_unit - ring_b)
        def _():
            pl.semaphore_signal(b_free, inc=1, device_id={'ep': x_peer}, device_id_type=MESH)

    tabulate()
    pl.semaphore_wait(barrier, n_ep)
    meta_copy.start()
    for o in range(1, n_ep):
        table_copy(o, me).start()
    tables[me] = table_mine[...]
    ahead = nk

    def phase_one(u, _):
        @pl.when(u < n_unit)
        def _():
            partial_sums(u)

        @pl.when((u >= 4) & (u < 4 + n_w))
        def _():
            start_tile(u - 4)

        @pl.when(u >= 1)
        def _():
            across_x(u - 1)

        @pl.when((u >= 2) & (lax.rem(u, 2) == 0))
        def _():
            across_y(u // 2 - 1)

        return 0

    lax.fori_loop(0, n_unit + 1, phase_one, 0)

    def attend(hp):
        abuf[:, col(hp, bn)] = head_mix(head_probs(head_scores(q_scr[...], k_scr[...]), seq_len), v_scr[...])


    def by_heads(hp):
        return (hp + 1) * 9 // 16

    def by_tiles(i):
        return by_heads(n_hp - 1) + (i + 1) * 5 // (n_ot // 2)

    n_last = nk - by_tiles(n_ot // 2 - 1)

    def pass_on(first, last):
        def unit(v, _):
            across_y(nk + v)
            return 0

        lax.fori_loop(first, last, unit, 0)

    def finish_waits(t):
        z_copy(t).wait_recv()

        @pl.when(t >= ring_o)
        def _():
            out_copy(t - ring_o).wait()

    def finish_sum(t):
        mine = pl.ds(pl.multiple_of(core * rows_g, rows_g), rows_g)
        proj = (zscr[lax.rem(t, ring_z), mine, :] + recv_z[lax.rem(t, ring_r)]).astype(BF16)
        zout[lax.rem(t, ring_o)] = (y_own[t // n_ot, :, col(lax.rem(t, n_ot), bn)].astype(F32) + proj.astype(F32)).astype(BF16)

    def finish_starts(t):
        out_copy(t).start()

        @pl.when(t < 2 * n_ot - ring_r)
        def _():
            pl.semaphore_signal(z_free, inc=1, device_id={'ep': core_peer}, device_id_type=MESH)

    def finish(t):
        finish_waits(t)
        finish_sum(t)
        finish_starts(t)

    def group_pass(g, _):
        @pl.when(g == 1)
        def _():
            pass_on(nk - n_last, nk)

        def arrived(k, _):
            for h in range(2):
                c_copy(g * nk + k, h).wait_recv()
            return 0

        lax.fori_loop(0, nk, arrived, 0)

        def norm(p, _):
            for half in range(2):
                y = y_own[g, pl.ds(pl.multiple_of(p * 32 + half * 16, 16), 16), :].astype(F32)
                inv = lax.rsqrt(jnp.mean(y * y, axis=1, keepdims=True) + NORM_EPS)
                xbuf[g, pl.ds(pl.multiple_of(core * rows_g + p * 32 + half * 16, 16), 16), :] = (y * inv * nw_ref[...]).astype(BF16)
            x_copy(g, p).start()
            return 0

        lax.fori_loop(0, rows_g // 32, norm, 0)

        def exchanged(p, _):
            x_copy(g, p).wait()
            return 0

        mine = pl.ds(pl.multiple_of(core * rows_g, rows_g), rows_g)
        theirs = pl.ds(pl.multiple_of((1 - core) * rows_g, rows_g), rows_g)
        first = g * n_tile

        def project_half(rows):
            for kind, scr in enumerate((q_scr, k_scr, v_scr)):
                scr[rows, :] = jnp.dot(xbuf[g, rows, :], wbuf[lax.rem(first + kind, n_w)], preferred_element_type=F32).astype(BF16)

        for kind in range(3):
            qkv_tile(first + kind, 0, kind).wait()
        project_half(mine)
        lax.fori_loop(0, rows_g // 32, exchanged, 0)
        project_half(theirs)
        for kind in range(3):
            start_tile(first + kind + n_w)

        def heads(hp, _):
            s = g * n_tile + hp * 3
            for kind in range(3):
                qkv_tile(s + kind, hp, kind).wait()
            scores = head_scores(q_scr[...], k_scr[...])
            q = jnp.dot(xbuf[g], wbuf[lax.rem(s, n_w)], preferred_element_type=F32).astype(BF16)
            mixed = head_mix(head_probs(scores, seq_len), v_scr[...])
            k = jnp.dot(xbuf[g], wbuf[lax.rem(s + 1, n_w)], preferred_element_type=F32).astype(BF16)
            v = jnp.dot(xbuf[g], wbuf[lax.rem(s + 2, n_w)], preferred_element_type=F32).astype(BF16)
            abuf[:, col(hp - 1, bn)] = mixed
            q_scr[...] = q
            k_scr[...] = k
            v_scr[...] = v
            for kind in range(3):
                start_tile(s + kind + n_w)

            @pl.when(g == 0)
            def _():
                pass_on(jnp.where(hp == 1, 0, by_heads(hp - 1)), by_heads(hp))

            return 0

        lax.fori_loop(1, n_hp, heads, 0)
        attend(n_hp - 1)

        def project(i, _):
            t = g * n_ot + 2 * i
            s = g * n_tile + 3 * n_hp + 2 * i

            def multiply():
                z = [jnp.dot(abuf[...], wbuf[lax.rem(s + r, n_w), 0:width, :], preferred_element_type=F32) for r in range(2)]
                for r in range(2):
                    zscr[lax.rem(t + r, ring_z)] = z[r]

            for r in range(2):
                @pl.when(t >= ring_z)
                def _():
                    z_copy(t + r - ring_z).wait_send()

                out_tile(s + r, 2 * i + r).wait()

            multiply()
            for r in range(2):
                start_tile(s + r + n_w)

                @pl.when(t >= ring_r)
                def _():
                    pl.semaphore_wait(z_free, 1)

                z_copy(t + r).start()

            @pl.when(i >= 1)
            def _():
                finish(t - 2)
                finish(t - 1)

            @pl.when(g == 0)
            def _():
                pass_on(by_tiles(i - 1), by_tiles(i))

            return 0

        lax.fori_loop(0, n_ot // 2, project, 0)
        finish(g * n_ot + n_ot - 2)
        finish(g * n_ot + n_ot - 1)
        return 0

    lax.fori_loop(0, 2, group_pass, 0)

    meta_copy.wait_send()
    for o in range(1, n_ep):
        table_copy(o, me).wait_send()
    for u in range(n_unit - 2, n_unit):
        a_copy(u).wait_send()
    for u in range(n_unit - ring_b, n_unit):
        for h in range(2):
            b_copy(u, h).wait_send()
    for u in range(n_unit - ring_c, n_unit):
        for h in range(2):
            c_copy(u, h).wait_send()
    for t in range(2 * n_ot - ring_z, 2 * n_ot):
        z_copy(t).wait_send()
    for t in range(2 * n_ot - ring_o, 2 * n_ot):
        out_copy(t).wait()


def stage(out_local, ids, slots, gate, owner, resid, norm_w, w_q, w_k, w_v, w_o, seq_len, n_ep, n_stages, dk=512, bn=256):
    n_exp, capacity, dim = out_local.shape
    n_tok = resid.shape[0]
    cap_dev = capacity // n_ep
    n_slot = n_exp * cap_dev
    width = w_q.shape[1] // 2
    rows_g = n_tok // 2
    n_unit = 2 * dim // dk
    n_w, ring_a, ring_b, ring_c, ring_z, ring_r, ring_o = 7, 3, 15, 2, 4, 4, 4
    any_spec = pl.BlockSpec(memory_space=pl.ANY)
    vmem_spec = pl.BlockSpec(memory_space=pltpu.VMEM)
    vmem, dma = pltpu.VMEM, pltpu.SemaphoreType.DMA
    return pl.pallas_call(
        functools.partial(stage_kernel, n_ep, n_stages, dk, bn, seq_len),
        out_shape=jax.ShapeDtypeStruct((n_tok, dim), BF16),
        in_specs=[any_spec, vmem_spec, vmem_spec, vmem_spec, vmem_spec, any_spec, vmem_spec] + [any_spec] * 4,
        out_specs=any_spec,
        scratch_shapes=[
            vmem((2 * ids.shape[0], n_tok), F32),
            vmem((owner.shape[1], 128), F32),
            vmem((n_ep, 2 * ids.shape[0], n_tok), F32),
            vmem((owner.shape[1], 128), F32),
            vmem((n_ep, n_exp, cap_dev, dk), BF16),
            vmem((n_tok, dk), BF16),
            vmem((n_ep, 3 * rows_g, n_slot), BF16),
            vmem((rows_g, n_tok), BF16),
            vmem((2, 2, rows_g, dk), F32),
            vmem((ring_a, 2, rows_g, dk), F32),
            vmem((ring_b, rows_g, dk), F32),
            vmem((ring_b, rows_g, dk), F32),
            vmem((ring_b, rows_g, dk), F32),
            vmem((ring_c, rows_g, dk), BF16),
            vmem((2, rows_g, dim), BF16),
            vmem((2, n_tok, dim), BF16),
            vmem((n_w, dim, bn), BF16),
            vmem((n_tok, width), BF16),
            vmem((n_tok, bn), BF16), vmem((n_tok, bn), BF16), vmem((n_tok, bn), BF16),
            vmem((ring_z, n_tok, bn), F32),
            vmem((ring_r, rows_g, bn), F32),
            vmem((ring_o, rows_g, bn), BF16),
            dma((n_ep,)), dma((1,)), dma((2,)), dma((ring_a,)), dma((2 * ring_b,)), dma((2 * ring_b,)), dma((2 * ring_c,)), dma((2 * n_unit,)),
            dma((rows_g // 32,)), dma((2 * rows_g // 32,)), dma((n_w,)), dma((ring_z,)), dma((ring_r,)), dma((ring_o,)),
            dma((n_ep,)), dma((n_ep,)), dma((1,)), dma((1,)),
            pltpu.SemaphoreType.REGULAR, pltpu.SemaphoreType.REGULAR, pltpu.SemaphoreType.REGULAR,
        ],
        compiler_params=pltpu.CompilerParams(collective_id=0, has_side_effects=True, vmem_limit_bytes=VMEM_LIMIT),
        name='stage',
    )(out_local, ids, slots, gate, owner, resid, norm_w, w_q, w_k, w_v, w_o)


def head_tiles(n_tok, width, blk):
    return [(slice(t * blk, (t + 1) * blk), slice(h * HEAD_DIM, (h + 1) * HEAD_DIM)) for h in range(width // HEAD_DIM) for t in range(n_tok // blk)]


def head_scores(q, k, blk=128):
    return [lax.dot_general(q[at], k[at], (((1,), (1,)), ((), ())), preferred_element_type=F32) for at in head_tiles(*q.shape, blk)]


def head_probs(scores, seq_len):
    blk = scores[0].shape[0]
    row = lax.broadcasted_iota(jnp.int32, (blk, blk), 0)
    col = lax.broadcasted_iota(jnp.int32, (blk, blk), 1)
    seen = (row >= col) & (row // seq_len == col // seq_len)
    probs = []
    for s in scores:
        s = jnp.where(seen, s * (HEAD_DIM ** -0.5), -1e30)
        e = jnp.exp(s - jnp.max(s, axis=1, keepdims=True))
        probs.append((e / jnp.sum(e, axis=1, keepdims=True)).astype(BF16))
    return probs


def head_mix(probs, v):
    n_tok, width = v.shape
    blk = probs[0].shape[0]
    tiles = [jnp.dot(p, v[at], preferred_element_type=F32).astype(BF16) for p, at in zip(probs, head_tiles(n_tok, width, blk))]
    per_head = n_tok // blk
    return jnp.concatenate([jnp.concatenate(tiles[h * per_head:(h + 1) * per_head], axis=0) for h in range(width // HEAD_DIM)], axis=1)


def place_kernel(seq_len, n_ep, own_ref, z_hbm, out_hbm, buf, in_sem, out_sem):
    n_seq = buf.shape[0]
    me = lax.axis_index('ep')
    sender = [own_ref[0, me * n_seq + b] // n_seq for b in range(n_seq)]

    def take(b):
        second = sum([(sender[a] == sender[b]).astype(jnp.int32) for a in range(b)], jnp.int32(0))
        row = pl.multiple_of((second * n_ep + sender[b]) * seq_len, seq_len)
        return pltpu.make_async_copy(z_hbm.at[pl.ds(row, seq_len)], buf.at[b], in_sem.at[b])

    def put(b):
        return pltpu.make_async_copy(buf.at[b], out_hbm.at[pl.ds(b * seq_len, seq_len)], out_sem.at[b])

    for b in range(n_seq):
        take(b).start()
    for b in range(n_seq):
        take(b).wait()
        put(b).start()
    for b in range(n_seq):
        put(b).wait()


def place_sequences(owner, z, seq_len, n_ep):
    n_tok, dim = z.shape
    n_seq = n_tok // seq_len
    return pl.pallas_call(
        functools.partial(place_kernel, seq_len, n_ep),
        in_specs=[pl.BlockSpec(memory_space=pltpu.SMEM), pl.BlockSpec(memory_space=pl.ANY)],
        out_specs=pl.BlockSpec(memory_space=pl.ANY),
        out_shape=jax.ShapeDtypeStruct((n_tok, dim), BF16),
        scratch_shapes=[pltpu.VMEM((n_seq, seq_len, dim), BF16), pltpu.SemaphoreType.DMA((n_seq,)), pltpu.SemaphoreType.DMA((n_seq,))],
        name='place_sequences',
    )(owner, z)


def solution(mesh):
    n_stages = mesh.shape['pp']
    n_ep = mesh.shape['ep']
    assert n_stages == 2 and n_ep == 4
    group_axes = ('data', 'pp')

    def device_step(expert_out, expert_id, slot_id, gate, resid, owner, norm_w, w_q, w_k, w_v, w_o):
        n_tok = resid.shape[2]
        seq_len = n_tok * n_ep // owner.shape[1]
        z = stage(expert_out[0, 0], expert_id[0, 0].T, slot_id[0, 0].T, gate[0, 0].T, owner, resid[0, 0], norm_w, w_q[0], w_k[0], w_v[0], w_o[0],
                  seq_len, n_ep, n_stages)
        return place_sequences(owner, z, seq_len, n_ep)[None, None]

    tok_spec = P(group_axes, None, 'ep', None)
    weight_spec = P('pp', None, None)
    in_specs = (P(group_axes, None, 'ep', None, None), tok_spec, tok_spec, tok_spec, tok_spec, P(group_axes, None), P('pp', None), weight_spec,
                weight_spec, weight_spec, weight_spec)
    return jax.shard_map(device_step, mesh=mesh, in_specs=in_specs, out_specs=tok_spec, check_vma=False)
```
